512 devices in a mesh: fsdp: 64 (over z, y), rep: 8 (over x, core).
Axes of the slice: x: 4, y: 8, z: 8, core: 2. Of those that a mesh axis runs over, the one named last changes fastest.
Arguments:
- params: float32 [24576, 3584], P(('fsdp', 'rep')), may hold values from -6 to 6
- grads: bfloat16 [24576, 3584], P(('fsdp', 'rep')), may hold values from -6 to 6
- moments: bfloat16 [3, 24576, 3584], P(None, ('fsdp', 'rep')), may hold values from -6 to 6
- row_acc: float32 [24576], P(('fsdp', 'rep')), may hold values from 0.05 to 1
- lengths: int32 [128], replicated, may hold values from 1 to 384, 24576 in all
- tensor_order: int32 [128], replicated, may hold values from 0 to 127, each once
- col_acc: float32 [128, 3584], P('fsdp'), may hold values from 0.05 to 1
- hidden_state: float32 [128, 512], P('fsdp'), may hold values from -1 to 1
- cell_state: float32 [128, 512], P('fsdp'), may hold values from -4 to 4
- lstm_in: bfloat16 [10, 2048], replicated, may hold values from -2 to 2
- lstm_rec: bfloat16 [512, 2048], replicated, may hold values from -0.25 to 0.25
- lstm_bias: float32 [2048], replicated, may hold values from -3 to 3
- hyper_first: bfloat16 [512, 256], replicated, may hold values from -0.25 to 0.25
- hyper_rest: bfloat16 [512, 128], replicated, may hold values from -0.25 to 0.25
Outputs:
- update: float32 [24576, 3584], P(('fsdp', 'rep'))
- row_new: float32 [24576], P(('fsdp', 'rep'))
- col_new: float32 [128, 3584], P('fsdp')
- hidden_new: float32 [128, 512], P('fsdp')
- cell_new: float32 [128, 512], P('fsdp')
The draws below stay inside these ranges and needn't reach their ends.
Inputs may be any that keep to these rules, and one draw needn't show every extreme that they name: `lengths`: they sum to 24576; the largest is 384. `tensor_order`: owner slot i belongs to fsdp index i // 2; each tensor appears once.
All inputs are finite; a program needn't handle non-finite values.
Results may differ from the reference program's by a relative error of at most 0.019.
Values may be sent and summed in bfloat16 or wider, within the bound.
A program may use at most 64 MiB of HBM per device.

```python
import math
import jax
import jax.numpy as jnp
import numpy as np
from jax import lax

C = 3584
HID = 512
FIN = 8
HM = 32
OUT = 3
FT = 10
NT = 128
ROWS = 24576
MOST = 384


def column_levels(key):
    exponent = jax.random.uniform(jax.random.fold_in(key, 71), (C,), jnp.float32, -1.5, 1.5)
    return jnp.exp(exponent)


def draw_grads(key, part):
    levels = column_levels(key)
    draw_key = jax.random.fold_in(key, 101)
    random_part = jax.random.normal(draw_key, (ROWS, C), jnp.float32)
    return jnp.clip(random_part * levels[None, :], -6.0, 6.0).astype(jnp.bfloat16)


def draw_col_acc(key, part):
    levels = column_levels(key)
    slot_exponent = jax.random.uniform(jax.random.fold_in(key, 201), (NT, 1), jnp.float32, jnp.log(0.1), jnp.log(0.4))
    jitter_key = jax.random.fold_in(key, 203)
    jitter = 0.3 * jax.random.normal(jitter_key, (NT, C), jnp.float32)
    values = jnp.exp(slot_exponent + jitter) * (levels * levels)[None, :]
    return jnp.clip(values, 0.05, 1.0).astype(jnp.float32)


def block_levels(key, shape, cuts, smallest, largest):
    level = 1.0
    for axis_at, blocks in cuts:
        steps = jax.random.uniform(jax.random.fold_in(jax.random.fold_in(key, 6), axis_at), (blocks,), jnp.float32, smallest / len(cuts), largest / len(cuts))
        level = level * jnp.repeat(jnp.exp(steps), shape[axis_at] // blocks).reshape((-1,) + (1,) * (len(shape) - 1 - axis_at))
    return level


def split_up(number_of, total, reach, slope):
    portions = [(1 << 20) // math.isqrt(grade ** slope) + 1 for grade in range(2, number_of + 1)]
    rest, holding = total - reach - (number_of - 1), [1] * (number_of - 1)
    while rest > 0:
        candidates = [i for i in range(number_of - 1) if holding[i] < reach]
        mass, budget = sum([portions[i] for i in candidates]), rest
        for i in candidates:
            more = min(reach - holding[i], max(1, budget * portions[i] // mass), rest)
            holding[i] = holding[i] + more
            rest = rest - more
    return np.array([reach] + holding)


def uneven(stream_key, number_of, total, bound, slope):
    if number_of == 2:
        one = jax.random.randint(stream_key, (), max(1, total - bound), min(bound, total - 1) + 1)
        return jnp.stack([one, total - one])
    tallies = jnp.asarray(split_up(number_of, total, bound, slope), jnp.int32)
    pairs = (number_of - 1) // 2
    donor, sink = tallies[1:1 + 2 * pairs:2], tallies[2:2 + 2 * pairs:2]
    slack = jnp.minimum(donor - 1, bound - sink)
    shifted = jax.random.randint(jax.random.fold_in(stream_key, 1), (pairs,), 0, 1 << 20) % (slack + 1)
    tallies = tallies.at[1:1 + 2 * pairs:2].set(donor - shifted).at[2:2 + 2 * pairs:2].set(sink + shifted)
    return tallies[jax.random.permutation(jax.random.fold_in(stream_key, 2), number_of)]


def centred(stream_key, shape, width, most, split=(), held_as=jnp.bfloat16):
    result = width * jax.random.normal(stream_key, shape, jnp.float32)
    if split:
        result = result * block_levels(stream_key, shape, split, -0.22, 0.18)
    return jnp.clip(result, -most, most).astype(held_as)


def setup_inputs(seed: int = 0) -> dict:
    key_list = jax.random.split(jax.random.key(seed), 15)
    params = centred(key_list[0], (ROWS, C), 1.0, 6.0, ((0, 512),), jnp.float32)
    grads = draw_grads(jax.random.fold_in(key_list[14], 71), 0)
    moments = centred(key_list[2], (3, ROWS, C), 1.0, 6.0, ((1, 512),))
    row_acc = jnp.clip(jnp.exp(math.log(1.0) - 2.9957323 * jax.random.uniform(key_list[3], (ROWS,), jnp.float32) ** block_levels(key_list[3], (ROWS,), ((0, 512),), -0.2, 0.2)), 0.05, 1.0)
    lengths = uneven(key_list[4], NT, ROWS, MOST, 2).astype(jnp.int32)
    tensor_order = jax.random.permutation(key_list[5], NT).astype(jnp.int32)
    col_acc = draw_col_acc(jax.random.fold_in(key_list[14], 71), 0)
    hidden_state = jnp.clip(jax.random.uniform(key_list[7], (NT, HID), jnp.float32, -1.0, 1.0) * block_levels(key_list[7], (NT, HID), ((0, 64),), -0.4, 0.0), -1.0, 1.0)
    cell_state = centred(key_list[8], (NT, HID), 1.0, 4.0, ((0, 64),), jnp.float32)
    lstm_in = centred(key_list[9], (FT, 4 * HID), FT ** -0.5, 2.0)
    lstm_rec = centred(key_list[10], (HID, 4 * HID), HID ** -0.5, 0.25)
    lstm_bias = centred(key_list[11], (4 * HID,), 0.5, 3.0, (), jnp.float32)
    hyper_first = centred(key_list[12], (HID, FIN * HM), HID ** -0.5, 0.25)
    hyper_rest = centred(key_list[13], (HID, HM * (1 + OUT)), HID ** -0.5, 0.25)
    return {"params": params, "grads": grads, "moments": moments, "row_acc": row_acc, "lengths": lengths, "tensor_order": tensor_order, "col_acc": col_acc, "hidden_state": hidden_state, "cell_state": cell_state, "lstm_in": lstm_in, "lstm_rec": lstm_rec, "lstm_bias": lstm_bias, "hyper_first": hyper_first, "hyper_rest": hyper_rest}


EPSILON = 1e-06
DECAY_RATE = 0.9

def owner_step(col_sums, tensor_stats, row_lengths, col_acc, hidden_state, cell_state, lstm_in, lstm_rec, lstm_bias, hyper_first, hyper_rest):
    col_width = col_acc.shape[1]
    col_new = DECAY_RATE * col_acc + (1.0 - DECAY_RATE) * col_sums / row_lengths[:, None]
    tensor_means = tensor_stats / (row_lengths * col_width)[:, None]
    log_means = jnp.log(tensor_means[:, :5] + EPSILON)
    corr_first = tensor_means[:, 5] / jnp.sqrt(tensor_means[:, 0] * tensor_means[:, 1] + EPSILON)
    corr_second = tensor_means[:, 6] / jnp.sqrt(tensor_means[:, 0] * tensor_means[:, 3] + EPSILON)
    corr_third = tensor_means[:, 7] / jnp.sqrt(tensor_means[:, 1] * tensor_means[:, 3] + EPSILON)
    col_mean = lax.optimization_barrier(jnp.mean(col_new, axis=1))
    col_square = lax.optimization_barrier(jnp.mean(col_new * col_new, axis=1))
    spread = jnp.log(col_square / (col_mean * col_mean))
    extra = jnp.stack([corr_first, corr_second, corr_third, jnp.log(col_mean + EPSILON), spread], axis=1)
    features = jnp.concatenate([log_means, extra], axis=1).astype(jnp.bfloat16)
    gate_sum = jnp.dot(features, lstm_in, preferred_element_type=jnp.float32)
    gate_sum = gate_sum + jnp.dot(hidden_state.astype(jnp.bfloat16), lstm_rec, preferred_element_type=jnp.float32) + lstm_bias
    hid_width = hidden_state.shape[1]
    gate_in = gate_sum[:, :hid_width]
    gate_forget = gate_sum[:, hid_width:2 * hid_width]
    gate_cand = gate_sum[:, 2 * hid_width:3 * hid_width]
    gate_out = gate_sum[:, 3 * hid_width:]
    cell_new = jax.nn.sigmoid(gate_forget) * cell_state + jax.nn.sigmoid(gate_in) * jnp.tanh(gate_cand)
    hidden_new = jax.nn.sigmoid(gate_out) * jnp.tanh(cell_new)
    hidden_bf = hidden_new.astype(jnp.bfloat16)
    gen_first = jnp.dot(hidden_bf, hyper_first, preferred_element_type=jnp.float32).astype(jnp.bfloat16)
    gen_rest = jnp.dot(hidden_bf, hyper_rest, preferred_element_type=jnp.float32).astype(jnp.bfloat16)
    tensor_scales = jnp.stack([jnp.sqrt(tensor_means[:, 0] + EPSILON), jnp.sqrt(tensor_means[:, 1] + EPSILON), jnp.sqrt(tensor_means[:, 4] + EPSILON), col_mean], axis=1)
    return (col_new, hidden_new, cell_new, gen_first, gen_rest, tensor_scales)

def param_block(param_rows, grad_rows, moment_rows, row_var, col_rows, first_rows, rest_rows, scale_rows):
    block_rows = param_rows.shape[0]
    grad_f = grad_rows.astype(jnp.float32)
    mom_f = moment_rows.astype(jnp.float32)
    v_factored = row_var[:, None] * col_rows / scale_rows[:, 3:4]
    inv_rms = lax.rsqrt(v_factored + EPSILON)
    grad_norm = grad_f * inv_rms
    mom_norm = mom_f[0] * inv_rms
    inputs = jnp.stack([grad_norm, mom_norm, mom_f[1] * inv_rms, mom_f[2] * inv_rms, grad_f / scale_rows[:, 0:1], mom_f[0] / scale_rows[:, 1:2], param_rows / scale_rows[:, 2:3], grad_norm * mom_norm], axis=1).astype(jnp.bfloat16)
    hm_width = rest_rows.shape[1] // 4
    w_first = first_rows.astype(jnp.float32).reshape(block_rows, 8, hm_width)
    bias_first = rest_rows[:, :hm_width].astype(jnp.float32)
    w_second = rest_rows[:, hm_width:].astype(jnp.float32).reshape(block_rows, hm_width, 3)
    hidden_units = jnp.einsum('bfc,bfh->bhc', inputs.astype(jnp.float32), w_first) + bias_first[:, :, None]
    hidden_units = jax.nn.relu(hidden_units).astype(jnp.bfloat16)
    mlp_out = jnp.einsum('bhc,bho->boc', hidden_units.astype(jnp.float32), w_second)
    return mlp_out[:, 0] * jnp.exp(jnp.tanh(mlp_out[:, 1])) * jax.nn.sigmoid(mlp_out[:, 2])

def reference(params, grads, moments, row_acc, lengths, tensor_order, col_acc, hidden_state, cell_state, lstm_in, lstm_rec, lstm_bias, hyper_first, hyper_rest):
    row_count = params.shape[0]
    tensor_count = lengths.shape[0]
    tensor_ends = jnp.cumsum(lengths).astype(jnp.int32)
    row_ids = jnp.arange(row_count, dtype=jnp.int32)
    seg_ids = lax.optimization_barrier(jnp.sum((row_ids[:, None] >= tensor_ends[None, :]).astype(jnp.int32), axis=1))
    grad_f = grads.astype(jnp.float32)
    grad_sq = grad_f * grad_f
    row_new = DECAY_RATE * row_acc + (1.0 - DECAY_RATE) * lax.optimization_barrier(jnp.mean(grad_sq, axis=1))
    mom_zero = moments[0].astype(jnp.float32)
    mom_one = moments[1].astype(jnp.float32)
    mom_two = moments[2].astype(jnp.float32)
    per_row = jnp.stack([lax.optimization_barrier(jnp.sum(grad_sq, axis=1)), lax.optimization_barrier(jnp.sum(mom_zero * mom_zero, axis=1)), lax.optimization_barrier(jnp.sum(mom_one * mom_one, axis=1)), lax.optimization_barrier(jnp.sum(mom_two * mom_two, axis=1)), lax.optimization_barrier(jnp.sum(params * params, axis=1)), lax.optimization_barrier(jnp.sum(grad_f * mom_zero, axis=1)), lax.optimization_barrier(jnp.sum(grad_f * mom_two, axis=1)), lax.optimization_barrier(jnp.sum(mom_zero * mom_two, axis=1))], axis=1)
    tensor_stats = jax.ops.segment_sum(per_row, seg_ids, num_segments=tensor_count)
    col_sums = jax.ops.segment_sum(grad_sq, seg_ids, num_segments=tensor_count)
    row_lengths = lengths[tensor_order].astype(jnp.float32)
    col_new, hidden_new, cell_new, gen_first, gen_rest, tensor_scales = owner_step(col_sums[tensor_order], tensor_stats[tensor_order], row_lengths, col_acc, hidden_state, cell_state, lstm_in, lstm_rec, lstm_bias, hyper_first, hyper_rest)
    col_table = jnp.zeros_like(col_new).at[tensor_order].set(col_new)
    first_table = jnp.zeros_like(gen_first).at[tensor_order].set(gen_first)
    rest_table = jnp.zeros_like(gen_rest).at[tensor_order].set(gen_rest)
    scale_table = jnp.zeros_like(tensor_scales).at[tensor_order].set(tensor_scales)
    block_rows = 64
    block_count = row_count // block_rows

    def one_block(index):
        start = (index * block_rows).astype(jnp.int32)
        seg_block = lax.dynamic_slice_in_dim(seg_ids, start, block_rows, 0)
        return param_block(lax.dynamic_slice_in_dim(params, start, block_rows, 0), lax.dynamic_slice_in_dim(grads, start, block_rows, 0), lax.dynamic_slice_in_dim(moments, start, block_rows, 1), lax.dynamic_slice_in_dim(row_new, start, block_rows, 0), col_table[seg_block], first_table[seg_block], rest_table[seg_block], scale_table[seg_block])
    update = lax.map(one_block, jnp.arange(block_count, dtype=jnp.int32)).reshape(params.shape)
    return (update, row_new, col_new, hidden_new, cell_new)
```

```python
import functools
import math

import jax
import jax.numpy as jnp
from jax import lax
from jax.experimental import pallas as pl
from jax.experimental.pallas import tpu as pltpu
from jax.sharding import PartitionSpec as P

EPS = 1e-06
DECAY = 0.9
FIN = 8
F32 = jnp.float32
BF16 = jnp.bfloat16
MESH = pl.DeviceIdType.MESH
VMEM = pltpu.VMEM
LIMIT = 60 * 1024 * 1024


class Sizes:
    def __init__(self, mesh, params, col_acc, hidden_state, rest):
        self.fsdp, self.rep = mesh.shape["fsdp"], mesh.shape["rep"]
        self.nz = self.ny = math.isqrt(self.fsdp)
        self.nt = col_acc.shape[0]
        self.own = self.nt // self.fsdp
        self.rows = params.shape[0] // (self.fsdp * self.rep)
        self.c = params.shape[1]
        self.hid = hidden_state.shape[1]
        self.hm = rest.shape[1] // 4
        self.sl = self.c // (self.rep - 1)
        self.cw = self.c + 128
        self.w = (self.c + 3 * self.hid) // 2
        self.all_rows = self.rows + 8
        assert self.own == 2 and self.sl % 128 == 0 and self.w % 128 == 0 and self.rows % 16 == 0


def iota(shape, dim):
    return lax.broadcasted_iota(jnp.int32, shape, dim)


def fiota(shape, dim):
    return iota(shape, dim).astype(F32)


def rem(a, b):
    return lax.rem(a, jnp.int32(b))


def div(a, b):
    return lax.div(a, jnp.int32(b))


def slot_bounds(s, lens, order):
    a, b = iota((s.nt, s.nt), 0), iota((s.nt, s.nt), 1)
    lens_col = jnp.sum(jnp.where(a == b, lens, 0.0), axis=1, keepdims=True)
    ids = a.astype(F32)
    end = jnp.sum(jnp.where(ids <= order, lens_col, 0.0), axis=0, keepdims=True)
    size = jnp.sum(jnp.where(ids == order, lens_col, 0.0), axis=0, keepdims=True)
    return end - size, end


def slot_hits(pos, start, end):
    return jnp.where((pos >= start) & (pos < end), 1.0, 0.0)


def ranges(pos, start, end):
    hits = slot_hits(pos, start, end)
    first = jnp.sum(hits * start, axis=1, keepdims=True)
    last = jnp.sum(hits * end, axis=1, keepdims=True)
    return first, last, hits


def split2(x):
    hi = x.astype(BF16)
    return hi, (x - hi.astype(F32)).astype(BF16)


def restack(t):
    lane = iota(t.shape, 1)
    both = t + pltpu.roll(t, 120, 1)
    hi = both.astype(BF16).astype(F32)
    low = pltpu.roll(both - hi, 8, 1)
    return jnp.where(lane < 8, hi, jnp.where(lane < 16, low, 0.0))


def local_kernel(s, params, grads, moments, row_acc, lens, order, col_acc, hidden, cell,
                 row_new, row_var, gs, ht, ag):
    device = lax.axis_index("fsdp") * s.rep + lax.axis_index("rep")
    start, end = slot_bounds(s, lens[...], order[...])
    own = jnp.concatenate([v.astype(BF16) for v in (col_acc[...], hidden[...])] + list(split2(cell[...])), axis=1)
    ag[0] = own[:, : s.w]
    ag[1] = own[:, s.w :]
    sums = [jnp.zeros((s.rows, 1), F32) for _ in range(8)]
    for j in range(s.rep - 1):
        cols = pl.ds(j * s.sl, s.sl)
        g, p = grads[:, cols].astype(F32), params[:, cols]
        m = [moments[k, :, cols].astype(F32) for k in range(3)]
        sq = g * g
        gs[j] = sq.astype(BF16)
        for k, v in enumerate((sq, m[0] * m[0], m[1] * m[1], m[2] * m[2], p * p, g * m[0], g * m[2], m[0] * m[2])):
            sums[k] = sums[k] + jnp.sum(v, axis=1, keepdims=True)
    lane = iota((s.rows, 128), 1)
    stats = jnp.zeros((s.rows, 128), F32)
    for k in range(8):
        hi, low = split2(sums[k])
        stats = jnp.where(lane == k, hi.astype(F32), stats)
        stats = jnp.where(lane == k + 8, low.astype(F32), stats)
    gs[s.rep - 1] = jnp.zeros((s.rows, s.sl), BF16)
    gs[s.rep - 1, :, :128] = stats.astype(BF16)
    a, b = iota((s.rows, s.rows), 0), iota((s.rows, s.rows), 1)
    acc_col = jnp.sum(jnp.where(a == b, row_acc[...], 0.0), axis=1, keepdims=True)
    new_col = DECAY * acc_col + (1.0 - DECAY) * (sums[0] / s.c)
    row_new[...] = jnp.sum(jnp.where(a == b, new_col, 0.0), axis=0, keepdims=True)
    row_var[...] = jnp.broadcast_to(new_col, (s.rows, 128))
    base = (device * s.rows).astype(F32)
    which = fiota((16, 1), 0)
    pos = jnp.where(which == 0.0, base, jnp.where(which == 1.0, base + (s.rows - 1), -1.0))
    first, last, _ = ranges(pos, start, end)
    here = base + fiota((1, s.rows), 1)
    pick = slot_hits(here, first, last).astype(BF16)
    for j in range(s.rep - 1):
        part = jnp.dot(pick, gs[j], preferred_element_type=F32)
        ht[:, j * s.sl : (j + 1) * s.sl] = part[:2].astype(BF16)
    part = jnp.dot(pick, gs[s.rep - 1, :, :128], preferred_element_type=F32)
    ht[:, s.c :] = restack(part)[:2].astype(BF16)


def remote(src, dst, sems, k, fsdp, rep):
    return pltpu.make_async_remote_copy(
        src_ref=src, dst_ref=dst, send_sem=sems.at[0, k], recv_sem=sems.at[1, k],
        device_id={"fsdp": fsdp, "rep": rep}, device_id_type=MESH,
    )


def comm_kernel(s, lens, order, ht, gs, ag, htall, nb, table, xbuf,
                piece, nbsrc, gx, zsrc, zbuf, ysrc, ybuf, xsrc,
                s_ht, s_nb, s_p, s_t, s_d, s_g, s_z, s_y, s_x):
    f, r = lax.axis_index("fsdp"), lax.axis_index("rep")
    z, y, core = div(f, s.ny), rem(f, s.ny), rem(r, 2)
    partner = r + 1 - 2 * core
    nxt, prv = rem(f + 1, s.fsdp), rem(f + s.fsdp - 1, s.fsdp)

    def at_rep(k):
        return rem(r + k, s.rep)

    def at_y(k):
        return z * s.ny + rem(y + k, s.ny)

    def at_z(k):
        return rem(z + k, s.nz) * s.ny + y

    def first_axis(k):
        return (1 - core) * at_y(k) + core * at_z(k)

    def second_axis(k):
        return (1 - core) * at_z(k) + core * at_y(k)

    barrier = pltpu.get_barrier_semaphore()
    peers = [(f, at_rep(k)) for k in range(1, s.rep)]
    peers += [(at_y(k), r) for k in range(1, s.ny)] + [(at_z(k), r) for k in range(1, s.nz)]
    peers += [(nxt, r), (prv, r)]
    for pf, pr in peers:
        pl.semaphore_signal(barrier, inc=1, device_id={"fsdp": pf, "rep": pr}, device_id_type=MESH)
    pl.semaphore_wait(barrier, len(peers))

    reps, ys, zs = range(1, s.rep), range(1, s.ny), range(1, s.nz)
    c_p = [remote(ag.at[core], piece.at[k], s_p, k, first_axis(k), r) for k in ys]
    c_ht = [remote(ht, htall.at[k], s_ht, k, f, at_rep(k)) for k in reps]
    c_g = [remote(gs.at[at_rep(k)], gx.at[k], s_g, k, f, at_rep(k)) for k in reps]
    for c in c_p + c_ht + c_g:
        c.start()
    htall[0] = ht[...]
    piece[0] = ag[core]
    gx[0] = gs[r]

    start, end = slot_bounds(s, lens[...], order[...])
    group = s.rep * s.rows
    base = (f * group).astype(F32)
    which = fiota((8, 1), 0)
    first, last, _ = ranges(jnp.where(which == 0.0, base + (group - 1), base), start, end)
    coef = []
    for k in range(s.rep):
        at = base + (rem(r + s.rep - k, s.rep) * s.rows).astype(F32)
        head = jnp.where((at >= first) & (at < last), 1.0, 0.0)
        tail = jnp.where((at + (s.rows - 1) >= first) & (at + (s.rows - 1) < last), 1.0, 0.0)
        coef.append((head, tail * (1.0 - head)))
    for c in c_ht:
        c.wait_recv()
    acc = jnp.zeros((2, s.cw), F32)
    for k in range(s.rep):
        both = htall[k].astype(F32)
        acc = acc + coef[k][0][:2] * both[0:1] + coef[k][1][:2] * both[1:2]
    acc = jnp.concatenate([acc[:, : s.c], restack(acc[:, s.c :])], axis=1)
    nbsrc[0] = jnp.broadcast_to(acc[0:1], (2, s.cw)).astype(BF16)
    nbsrc[1] = jnp.broadcast_to(acc[1:2], (2, s.cw)).astype(BF16)
    c_nb = [remote(nbsrc.at[0], nb.at[0], s_nb, 0, nxt, r), remote(nbsrc.at[1], nb.at[1], s_nb, 1, prv, r)]
    for c in c_nb:
        c.start()

    for c in c_p:
        c.wait_recv()
    table[core, 0] = jnp.concatenate([piece[k] for k in range(s.ny)], axis=0)
    c_t = [remote(table.at[core, 0], table.at[core, k], s_t, k, second_axis(k), r) for k in zs]
    c_d = [remote(table.at[core, k], table.at[core, k], s_d, k, f, partner) for k in range(s.nz)]
    for c in c_t + c_d[:1]:
        c.start()

    for c in c_g:
        c.wait_recv()
    per = 2 * s.ny
    a, b = iota((s.nt, s.nt), 0), iota((s.nt, s.nt), 1)
    slot = rem(rem(z + div(a, per), s.nz) * per + rem(a, per), s.nt)
    order_col = jnp.sum(jnp.where(b == slot, order[...], 0.0), axis=1, keepdims=True)
    ids = b.astype(F32)
    end_col = jnp.sum(jnp.where(ids <= order_col, lens[...], 0.0), axis=1, keepdims=True)
    start_col = end_col - jnp.sum(jnp.where(ids == order_col, lens[...], 0.0), axis=1, keepdims=True)
    sums = jnp.zeros((s.nt, s.sl), F32)
    for k in range(s.rep):
        at = base + (rem(r + s.rep - k, s.rep) * s.rows).astype(F32) + fiota((1, s.rows), 1)
        sums = sums + jnp.dot(slot_hits(at, start_col, end_col).astype(BF16), gx[k], preferred_element_type=F32)
    for k in range(s.nz):
        zsrc[k] = sums[k * per : (k + 1) * per].astype(BF16)
    c_z = [remote(zsrc.at[k], zbuf.at[k], s_z, k, at_z(k), r) for k in zs]
    for c in c_z:
        c.start()
    zbuf[0] = zsrc[0]

    for k in zs:
        c_t[k - 1].wait_recv()
        c_d[k].start()

    for c in c_z:
        c.wait_recv()
    total = zbuf[0].astype(F32)
    for k in zs:
        total = total + zbuf[k].astype(F32)
    ysrc[...] = total.astype(BF16)
    c_y = [remote(ysrc, ybuf.at[k], s_y, k, at_y(k), r) for k in ys]
    for c in c_y:
        c.start()
    for c in c_y:
        c.wait_recv()
    total = ysrc[...].astype(F32)
    for k in ys:
        total = total + ybuf[k].astype(F32)
    row = iota((per, s.sl), 0)
    mine = [jnp.sum(jnp.where(row == 2 * y + j, total, 0.0), axis=0, keepdims=True) for j in range(2)]
    row = iota((8, s.sl), 0)
    out = jnp.where(row == 0, mine[0], jnp.where(row == 1, mine[1], 0.0))
    xsrc[...] = out
    c_x = [remote(xsrc, xbuf.at[r], s_x, k, f, at_rep(k)) for k in reps]
    for c in c_x:
        c.start()
    xbuf[r] = out

    for c in c_x + c_d + c_nb:
        c.wait_recv()
    for c in c_p + c_ht + c_g + c_nb + c_t + c_d + c_z + c_y + c_x:
        c.wait_send()


def final_kernel(s, params, grads, moments, row_var, lens, order, col_acc, hidden, cell, w_in, w_rec, bias, w_first,
                 w_rest, gs, htall, nb, table, xbuf,
                 update, col_new, hidden_new, cell_new,
                 cols, ht16, gen, pick_w2):
    f, r = lax.axis_index("fsdp"), lax.axis_index("rep")
    z, y = div(f, s.ny), rem(f, s.ny)
    rows, n, nt, chunks = s.rows, s.all_rows, s.nt, s.rep - 1
    start, end = slot_bounds(s, lens[...], order[...])
    base = ((f * s.rep + r) * rows).astype(F32)
    row = iota((n, 1), 0)
    pos = jnp.where(row < rows, base + row.astype(F32), -1.0)
    lane = iota((n, nt), 1)
    mine = jnp.where((row >= rows) & (row < rows + 2) & (lane == row - rows + 2 * f), 1.0, 0.0)
    hits = slot_hits(pos, start, end) + mine
    first = jnp.sum(hits * start, axis=1, keepdims=True)
    last = jnp.sum(hits * end, axis=1, keepdims=True)
    length = jnp.maximum(last - first, 1.0)
    slot_of = jnp.sum(hits * lane.astype(F32), axis=1, keepdims=True)
    last = jnp.where(row < rows, last, first)

    group = (f * (s.rep * rows)).astype(F32)
    same = slot_hits(base + fiota((1, rows), 1), first, last).astype(BF16)
    la = iota((1, 2 * s.rep), 1)
    src = rem(r + s.rep - div(la, 2), s.rep)
    head = group + (src * rows).astype(F32)
    in_head = slot_hits(head, first, last)
    in_tail = slot_hits(head + (rows - 1), first, last) * (1.0 - in_head)
    shared = jnp.where(div(la, 2) == 0, 0.0, jnp.where(rem(la, 2) == 0, in_head, in_tail)).astype(BF16)
    before = slot_hits(group - 1.0, first, last)
    after = slot_hits(group + s.rep * rows, first, last)

    for k in range(s.rep):
        ht16[2 * k : 2 * k + 2, :] = htall[k].astype(F32)

    per = 2 * s.ny
    zz, yy, jj = div(lane, per), rem(div(lane, 2), s.ny), rem(lane, 2)
    slot_a = rem(z + s.nz - zz, s.nz) * per + rem(y + s.ny - yy, s.ny) * 2 + jj
    slot_b = rem(z + s.nz - yy, s.nz) * per + rem(y + s.ny - zz, s.ny) * 2 + jj
    hit_a = jnp.where(slot_a.astype(F32) == slot_of, 1.0, 0.0).astype(BF16)
    hit_b = jnp.where(slot_b.astype(F32) == slot_of, 1.0, 0.0).astype(BF16)
    top = iota((8, 1), 0)

    def own_rows(a):
        return jnp.where(top == 0, a[0:1], jnp.where(top == 1, a[1:2], 0.0))

    def held(lo, hi, own):
        parts = []
        for half, hit in ((0, hit_a), (1, hit_b)):
            a, b = max(lo, half * s.w) - half * s.w, min(hi, (half + 1) * s.w) - half * s.w
            if a < b:
                t = table[half, :, :, a:b].reshape(nt, b - a)
                parts.append(jnp.dot(hit[:rows], t, preferred_element_type=F32))
        got = parts[0] if len(parts) == 1 else jnp.concatenate(parts, axis=1)
        return jnp.concatenate([got, own_rows(own)], axis=0)

    def sums(g, lo, hi, total):
        out = jnp.dot(same[:rows], g, preferred_element_type=F32)
        out = out + jnp.dot(shared[:rows], ht16[: 2 * s.rep, lo:hi].astype(BF16), preferred_element_type=F32)
        out = out + before[:rows] * nb[0, :, lo:hi].astype(F32)[0:1] + after[:rows] * nb[1, :, lo:hi].astype(F32)[0:1]
        return jnp.concatenate([out, total], axis=0)

    total_col = jnp.zeros((n, 1), F32)
    total_sq = jnp.zeros((n, 1), F32)
    for j in range(chunks):
        lo, hi = j * s.sl, (j + 1) * s.sl
        got = sums(gs[j], lo, hi, xbuf[j])
        new = DECAY * held(lo, hi, col_acc[:, lo:hi]) + (1.0 - DECAY) * got / length
        cols[:, lo:hi] = new
        col_new[:, lo:hi] = new[rows : rows + 2]
        total_col = total_col + jnp.sum(new, axis=1, keepdims=True)
        total_sq = total_sq + jnp.sum(new * new, axis=1, keepdims=True)
    stats = sums(gs[chunks, :, :128], s.c, s.cw, xbuf[chunks, :, :128])
    means = [(stats[:, k : k + 1] + stats[:, k + 8 : k + 9]) / (length * s.c) for k in range(8)]
    col_mean = total_col / s.c
    col_square = total_sq / s.c
    feats = [jnp.log(means[k] + EPS) for k in range(5)]
    feats += [means[5] / jnp.sqrt(means[0] * means[1] + EPS), means[6] / jnp.sqrt(means[0] * means[3] + EPS),
              means[7] / jnp.sqrt(means[1] * means[3] + EPS), jnp.log(col_mean + EPS),
              jnp.log(col_square / (col_mean * col_mean))]
    feats = [v.astype(BF16).astype(F32) for v in feats]
    hid = held(s.c, s.c + s.hid, hidden[...]).astype(BF16)
    old = held(s.c + s.hid, s.c + 2 * s.hid, cell[...]) + held(s.c + 2 * s.hid, s.c + 3 * s.hid, jnp.zeros_like(cell[...]))

    def gate(k):
        lo, hi = k * s.hid, (k + 1) * s.hid
        out = jnp.dot(hid, w_rec[:, lo:hi], preferred_element_type=F32) + bias[:, lo:hi]
        w = w_in[:, lo:hi].astype(F32)
        for i, v in enumerate(feats):
            out = out + v * w[i : i + 1]
        return out

    now = jax.nn.sigmoid(gate(1)) * old + jax.nn.sigmoid(gate(0)) * jnp.tanh(gate(2))
    state = jax.nn.sigmoid(gate(3)) * jnp.tanh(now)
    hidden_new[...] = state[rows : rows + 2]
    cell_new[...] = now[rows : rows + 2]
    bf = state.astype(BF16)
    width = (FIN + 1 + 3) * s.hm
    gen[:, : FIN * s.hm] = jnp.dot(bf, w_first[...], preferred_element_type=F32)
    gen[:, FIN * s.hm :] = jnp.dot(bf, w_rest[...], preferred_element_type=F32)
    inv = [1.0 / jnp.sqrt(means[k][:rows] + EPS) for k in (0, 1, 4)]
    var = row_var[:, 0:1] / col_mean[:rows]

    m, deep = 8 * s.hm, 8 * (FIN + 2)
    lw = iota((m, width), 1)
    spread = jnp.where(rem(iota((m, 8), 0), 8) == iota((m, 8), 1), 1.0, 0.0).astype(BF16)
    keep = (rem(lw, s.hm) == div(iota((m, width), 0), 8)) & (lw < (FIN + 1) * s.hm)
    fold = jnp.where(div(iota((width, deep), 0), s.hm) == div(iota((width, deep), 1), 8), 1.0, 0.0).astype(BF16)
    diag1 = (rem(iota((m, deep), 0), 8) == rem(iota((m, deep), 1), 8)) & (iota((m, deep), 1) < 8 * (FIN + 1))
    diag2 = iota((8, m), 0) == rem(iota((8, m), 1), 8)
    for o in range(3):
        want = (FIN + 1) * s.hm + 3 * div(iota((width, m), 1), 8) + o
        pick_w2[o] = jnp.where(iota((width, m), 0) == want, 1.0, 0.0).astype(BF16)
    cols_scale = jnp.concatenate([var, inv[0], inv[1], inv[2]], axis=1)
    ht16[0:rows, 0:4] = cols_scale

    ones, zeros = jnp.ones((8, s.sl), F32), jnp.zeros((8, s.sl), F32)

    def block(i, carry):
        at = pl.multiple_of(i * 16, 16)
        made = gen[pl.ds(at, 16), :].astype(BF16).astype(F32)
        sc = ht16[pl.ds(at, 16), 0:128]
        weights = []
        for half in range(2):
            own = made[8 * half : 8 * half + 8].astype(BF16)
            y1 = jnp.where(keep, jnp.dot(spread, own, preferred_element_type=F32), 0.0).astype(BF16)
            w1 = jnp.where(diag1, jnp.dot(y1, fold, preferred_element_type=F32), 0.0).astype(BF16)
            w2 = [jnp.where(diag2, jnp.dot(own, pick_w2[o], preferred_element_type=F32), 0.0) for o in range(3)]
            weights.append((w1, jnp.concatenate(w2, axis=0).astype(BF16)))
        for j in range(chunks):
            lo, hi = j * s.sl, (j + 1) * s.sl
            g16 = grads[pl.ds(at, 16), lo:hi].astype(F32)
            m16 = [moments[k, pl.ds(at, 16), lo:hi].astype(F32) for k in range(3)]
            p16 = params[pl.ds(at, 16), lo:hi]
            c16 = cols[pl.ds(at, 16), lo:hi]
            for half in range(2):
                q = slice(8 * half, 8 * half + 8)
                g, m0, m1, m2, p, cn = g16[q], m16[0][q], m16[1][q], m16[2][q], p16[q], c16[q]
                rms = lax.rsqrt(cn * sc[q, 0:1] + EPS)
                gn, mn = g * rms, m0 * rms
                x = jnp.concatenate(
                    [gn, mn, m1 * rms, m2 * rms, g * sc[q, 1:2], m0 * sc[q, 2:3], p * sc[q, 3:4], gn * mn, ones, zeros],
                    axis=0,
                ).astype(BF16)
                w1, w2 = weights[half]
                unit = jnp.maximum(jnp.dot(w1, x, preferred_element_type=F32), 0.0).astype(BF16)
                o = jnp.dot(w2, unit, preferred_element_type=F32)
                out = o[0:8] * jnp.exp(jnp.tanh(o[8:16])) * jax.nn.sigmoid(o[16:24])
                update[pl.ds(pl.multiple_of(at + 8 * half, 8), 8), lo:hi] = out
        return carry

    lax.fori_loop(0, rows // 16, block, 0)


def on_device(s, params, grads, moments, row_acc, lengths, tensor_order, col_acc, hidden_state, cell_state,
              lstm_in, lstm_rec, lstm_bias, hyper_first, hyper_rest):
    shape = jax.ShapeDtypeStruct
    rows = s.rows
    lens = lengths.astype(F32).reshape(1, s.nt)
    order = tensor_order.astype(F32).reshape(1, s.nt)
    limit = pltpu.CompilerParams(vmem_limit_bytes=LIMIT)
    row_new, row_var, gs, ht, ag = pl.pallas_call(
        functools.partial(local_kernel, s),
        out_shape=(
            shape((1, rows), F32), shape((rows, 128), F32), shape((s.rep, rows, s.sl), BF16), shape((2, s.cw), BF16),
            shape((2, 2, s.w), BF16),
        ),
        compiler_params=limit,
        name="local",
    )(params, grads, moments, row_acc.reshape(1, rows), lens, order, col_acc, hidden_state, cell_state)

    def sems(k):
        return pltpu.SemaphoreType.DMA((2, k))

    per = 2 * s.ny
    htall, nb, table, xbuf = pl.pallas_call(
        functools.partial(comm_kernel, s),
        out_shape=(
            shape((s.rep, 2, s.cw), BF16), shape((2, 2, s.cw), BF16), shape((2, s.nz, per, s.w), BF16),
            shape((s.rep, 8, s.sl), F32),
        ),
        in_specs=[pl.BlockSpec(memory_space=VMEM)] * 5,
        out_specs=(pl.BlockSpec(memory_space=VMEM),) * 4,
        scratch_shapes=[
            VMEM((s.ny, 2, s.w), BF16), VMEM((2, 2, s.cw), BF16), VMEM((s.rep, rows, s.sl), BF16),
            VMEM((s.nz, per, s.sl), BF16), VMEM((s.nz, per, s.sl), BF16), VMEM((per, s.sl), BF16),
            VMEM((s.ny, per, s.sl), BF16), VMEM((8, s.sl), F32),
            sems(s.rep), sems(2), sems(s.ny), sems(s.nz), sems(s.nz), sems(s.rep), sems(s.nz), sems(s.ny), sems(s.rep),
        ],
        compiler_params=pltpu.CompilerParams(collective_id=0, has_side_effects=True, vmem_limit_bytes=LIMIT),
        name="exchange",
    )(lens, order, ht, gs, ag)
    width = (FIN + 4) * s.hm
    update, col_new, hidden_new, cell_new = pl.pallas_call(
        functools.partial(final_kernel, s),
        out_shape=(
            shape(params.shape, F32), shape(col_acc.shape, F32), shape(hidden_state.shape, F32),
            shape(cell_state.shape, F32),
        ),
        scratch_shapes=[
            VMEM((s.all_rows, s.c), F32), VMEM((max(2 * s.rep, rows), s.cw), F32), VMEM((s.all_rows, width), F32),
            VMEM((3, width, 8 * s.hm), BF16),
        ],
        compiler_params=limit,
        name="networks",
    )(params, grads, moments, row_var, lens, order, col_acc, hidden_state, cell_state, lstm_in, lstm_rec,
      lstm_bias.reshape(1, -1), hyper_first, hyper_rest, gs, htall, nb, table, xbuf)
    return update, row_new.reshape(rows), col_new, hidden_new, cell_new


def solution(mesh):
    rowwise, owned, everywhere = P(("fsdp", "rep"), None), P("fsdp", None), P()

    def step(params, grads, moments, row_acc, lengths, tensor_order, col_acc, hidden_state, cell_state, *weights):
        s = Sizes(mesh, params, col_acc, hidden_state, weights[-1])
        return jax.shard_map(
            functools.partial(on_device, s),
            mesh=mesh,
            in_specs=(rowwise, rowwise, P(None, ("fsdp", "rep"), None), P(("fsdp", "rep")), everywhere, everywhere,
                      owned, owned, owned) + (everywhere,) * 5,
            out_specs=(rowwise, P(("fsdp", "rep")), owned, owned, owned),
            check_vma=False,
        )(params, grads, moments, row_acc, lengths, tensor_order, col_acc, hidden_state, cell_state, *weights)

    return step
```

```python
import functools
import math

import jax
import jax.numpy as jnp
from jax import lax
from jax.experimental import pallas as pl
from jax.experimental.pallas import tpu as pltpu
from jax.sharding import PartitionSpec as P

EPS = 1e-06
DECAY = 0.9
FIN = 8
F32 = jnp.float32
BF16 = jnp.bfloat16
MESH = pl.DeviceIdType.MESH
VMEM = pltpu.VMEM
LIMIT = 60 * 1024 * 1024
ANY = pl.BlockSpec(memory_space=pltpu.HBM)


class Sizes:
    def __init__(self, mesh, params, col_acc, hidden_state, rest):
        self.fsdp, self.rep = mesh.shape["fsdp"], mesh.shape["rep"]
        self.nz = self.ny = math.isqrt(self.fsdp)
        self.nt = col_acc.shape[0]
        self.own = self.nt // self.fsdp
        self.rows = params.shape[0] // (self.fsdp * self.rep)
        self.c = params.shape[1]
        self.hid = hidden_state.shape[1]
        self.hm = rest.shape[1] // 4
        self.sl = self.c // (self.rep - 1)
        self.cw = self.c + 128
        self.q = -(-(self.c + 3 * self.hid) // 1024) * 128
        self.all_rows = self.rows + 8
        assert self.own == 2 and self.sl % 128 == 0 and self.rows % 16 == 0


def iota(shape, dim):
    return lax.broadcasted_iota(jnp.int32, shape, dim)


def fiota(shape, dim):
    return iota(shape, dim).astype(F32)


def rem(a, b):
    return lax.rem(a, jnp.int32(b))


def div(a, b):
    return lax.div(a, jnp.int32(b))


def slot_bounds(s, lens, order):
    a, b = iota((s.nt, s.nt), 0), iota((s.nt, s.nt), 1)
    lens_col = jnp.sum(jnp.where(a == b, lens, 0.0), axis=1, keepdims=True)
    ids = a.astype(F32)
    end = jnp.sum(jnp.where(ids <= order, lens_col, 0.0), axis=0, keepdims=True)
    size = jnp.sum(jnp.where(ids == order, lens_col, 0.0), axis=0, keepdims=True)
    return end - size, end


def slot_hits(pos, start, end):
    return jnp.where((pos >= start) & (pos < end), 1.0, 0.0)


def ranges(pos, start, end):
    hits = slot_hits(pos, start, end)
    first = jnp.sum(hits * start, axis=1, keepdims=True)
    last = jnp.sum(hits * end, axis=1, keepdims=True)
    return first, last, hits


def split2(x):
    hi = x.astype(BF16)
    return hi, (x - hi.astype(F32)).astype(BF16)


def restack(t):
    lane = iota(t.shape, 1)
    both = t + pltpu.roll(t, 120, 1)
    hi = both.astype(BF16).astype(F32)
    low = pltpu.roll(both - hi, 8, 1)
    return jnp.where(lane < 8, hi, jnp.where(lane < 16, low, 0.0))


def remote(src, dst, send_sem, recv_sem, fsdp, rep):
    return pltpu.make_async_remote_copy(
        src_ref=src, dst_ref=dst, send_sem=send_sem, recv_sem=recv_sem,
        device_id={"fsdp": fsdp, "rep": rep}, device_id_type=MESH,
    )


def log_features(means, col_mean, col_square):
    feats = [jnp.log(means[k] + EPS) for k in range(5)]
    feats += [means[5] / jnp.sqrt(means[0] * means[1] + EPS), means[6] / jnp.sqrt(means[0] * means[3] + EPS),
              means[7] / jnp.sqrt(means[1] * means[3] + EPS), jnp.log(col_mean + EPS),
              jnp.log(col_square / (col_mean * col_mean))]
    return [v.astype(BF16).astype(F32) for v in feats]


def cell_step(s, feats, rec, w_in, bias, old):
    def gate(k):
        lo, hi = k * s.hid, (k + 1) * s.hid
        out = rec(k) + bias[:, lo:hi]
        w = w_in[:, lo:hi].astype(F32)
        for i, v in enumerate(feats):
            out = out + v * w[i : i + 1]
        return out

    now = jax.nn.sigmoid(gate(1)) * old + jax.nn.sigmoid(gate(0)) * jnp.tanh(gate(2))
    return jax.nn.sigmoid(gate(3)) * jnp.tanh(now), now


def kernel(s, params_h, grads_h, moments_h, row_acc_h, lens_h, order_h, col_acc_h, hidden_h, cell_h, w_in_h, w_rec_h,
           bias_h, w_first_h, w_rest_h,
           update_h, row_new_h, col_new_h, hidden_new_h, cell_new_h,
           params, grads, moments, row_acc, lens_i, order_i, col_acc, hidden, cell, w_in, w_rec, bias, w_first, w_rest,
           s_in, s_big, s_w, s_out,
           gs, ht, ag, htall, nb, table, nbsrc, gx, zsrc, zbuf, ysrc, ybuf,
           sent, one_come, p_come, t_come, y_come,
           cols, ht16, gen, scales, pick_w2, own_rec, held, update, row_new, col_new, hidden_new, cell_new):
    f, r = lax.axis_index("fsdp"), lax.axis_index("rep")
    z, y, core = div(f, s.ny), rem(f, s.ny), rem(r, 2)
    partner = r + 1 - 2 * core
    nxt, prv = rem(f + 1, s.fsdp), rem(f + s.fsdp - 1, s.fsdp)
    rows, nt, chunks, per = s.rows, s.nt, s.rep - 1, 2 * s.ny
    reps, ys, zs = range(1, s.rep), range(1, s.ny), range(1, s.nz)

    def at_rep(k):
        return rem(r + k, s.rep)

    def at_y(k):
        return z * s.ny + rem(y + k, s.ny)

    def at_z(k):
        return rem(z + k, s.nz) * s.ny + y

    ht_k, g_k, z_k, d_k, nb_k, p_k, t_k, y_k, y0_k = range(9)

    def all_come(ref, kind, fsdp, rep):
        remote(ref, ref, sent.at[kind], one_come.at[kind], fsdp, rep).wait_recv()

    def first_axis(k):
        return (1 - core) * at_y(k) + core * at_z(k)

    def second_axis(k):
        return (1 - core) * at_z(k) + core * at_y(k)

    with jax.named_scope("greet"):
        def fetch(pairs, sem):
            made = [pltpu.make_async_copy(a, b, sem.at[i]) for i, (a, b) in enumerate(pairs)]
            for c in made:
                c.start()
            return made

        small = fetch([(col_acc_h, col_acc), (hidden_h, hidden), (cell_h, cell), (lens_h, lens_i), (order_h, order_i),
                       (row_acc_h, row_acc)], s_in)
        barrier = pltpu.get_barrier_semaphore()
        peers = [(at_z(k), 2 * x) for k in zs for x in range(s.rep // 2)]
        peers += [(at_y(k), 2 * x + 1) for k in ys for x in range(s.rep // 2)]
        peers += [(f, at_rep(k)) for k in reps] + [(first_axis(k), r) for k in ys] + [(nxt, r), (prv, r)]
        for pf, pr in peers:
            pl.semaphore_signal(barrier, inc=1, device_id={"fsdp": pf, "rep": pr}, device_id_type=MESH)
        big = fetch([(grads_h, grads)] + [(moments_h.at[k], moments.at[k]) for k in range(3)] + [(params_h, params)], s_big)
        weights = fetch([(w_rec_h, w_rec), (w_in_h, w_in), (bias_h, bias), (w_first_h, w_first), (w_rest_h, w_rest)], s_w)

    with jax.named_scope("own"):
        for c in small[:3]:
            c.wait()
        own = jnp.concatenate([v.astype(BF16) for v in (col_acc[...], hidden[...])] + list(split2(cell[...])), axis=1)
        if s.c + 3 * s.hid < 8 * s.q:
            own = jnp.concatenate([own, jnp.zeros((2, 8 * s.q - s.c - 3 * s.hid), BF16)], axis=1)
        own = own.astype(F32)
        for half in range(2):
            parts = [own[:, (4 * half + q) * s.q : (4 * half + q + 1) * s.q] for q in range(4)]
            ag[half] = jnp.concatenate(parts, axis=0).astype(BF16)
    with jax.named_scope("meet"):
        pl.semaphore_wait(barrier, len(peers))
        c_p = {k: remote(ag.at[core], table.at[core, 0, k], sent.at[p_k], p_come.at[k], first_axis(k), r) for k in ys}
        near = sorted(zs, key=lambda k: min(k, s.nz - k))
        ring = s.nz == 8
        early = (0, 1, 7, 2, 6) if ring else ()
        t_two = {}

        def hop(src, slot, piece, to):
            sem = t_come.at[8 + 2 * piece + (slot == 6)] if slot in (2, 6) and piece in early else t_come.at[slot]
            c = remote(src, table.at[core, slot, piece], sent.at[t_k], sem, second_axis(to), r)
            c.start()
            return c

        def pass_on(piece, src):
            for k in (2, 6, 1, 7) if piece in early else near[::-1]:
                t_two[k, piece] = hop(src, k, piece, k)

        def relay(piece):
            t_two[2, piece].wait_recv()
            if piece % 2 == 0:
                hop(table.at[core, 2, piece], 4, piece, 2)
            hop(table.at[core, 2, piece], 3, piece, 1)
            t_two[6, piece].wait_recv()
            if piece % 2 == 1:
                hop(table.at[core, 6, piece], 4, piece, 6)
            hop(table.at[core, 6, piece], 5, piece, 7)

        for k in near[::-1]:
            c_p[k].start()
        pass_on(0, ag.at[core])
        table[core, 0, 0] = ag[core]

    with jax.named_scope("stats"):
        for c in big:
            c.wait()
        sums = [jnp.zeros((rows, 1), F32) for _ in range(8)]
        for j in range(chunks):
            cs = pl.ds(j * s.sl, s.sl)
            g, p = grads[:, cs].astype(F32), params[:, cs]
            m = [moments[k, :, cs].astype(F32) for k in range(3)]
            sq = g * g
            gs[j] = sq.astype(BF16)
            for k, v in enumerate((sq, m[0] * m[0], m[1] * m[1], m[2] * m[2], p * p, g * m[0], g * m[2], m[0] * m[2])):
                sums[k] = sums[k] + jnp.sum(v, axis=1, keepdims=True)
        lane = iota((rows, 128), 1)
        stats = jnp.zeros((rows, 128), F32)
        for k in range(8):
            hi, low = split2(sums[k])
            stats = jnp.where(lane == k, hi.astype(F32), stats)
            stats = jnp.where(lane == k + 8, low.astype(F32), stats)
        gs[chunks] = jnp.zeros((rows, s.sl), BF16)
        gs[chunks, :, :128] = stats.astype(BF16)
    with jax.named_scope("send1"):
        c_g = [remote(gs.at[at_rep(k)], gx.at[k], sent.at[g_k], one_come.at[g_k], f, at_rep(k)) for k in reps]
        for c in c_g:
            c.start()
    with jax.named_scope("ends"):
        for c in small[3:]:
            c.wait()
        lens, order = lens_i[...].astype(F32), order_i[...].astype(F32)
        start, end = slot_bounds(s, lens, order)
        base = ((f * s.rep + r) * rows).astype(F32)
        which = fiota((16, 1), 0)
        pos = jnp.where(which == 0.0, base, jnp.where(which == 1.0, base + (rows - 1), -1.0))
        first, last, _ = ranges(pos, start, end)
        here = base + fiota((1, rows), 1)
        pick = slot_hits(here, first, last).astype(BF16)
        for j in range(chunks):
            part = jnp.dot(pick, gs[j], preferred_element_type=F32)
            ht[:, j * s.sl : (j + 1) * s.sl] = part[:2].astype(BF16)
        part = jnp.dot(pick, gs[chunks, :, :128], preferred_element_type=F32)
        ht[:, s.c :] = restack(part)[:2].astype(BF16)
        c_ht = [remote(ht, htall.at[k], sent.at[ht_k], one_come.at[ht_k], f, at_rep(k)) for k in reps]
        for c in c_ht:
            c.start()
        htall[0] = ht[...]
        gx[0] = gs[r]
        a, b = iota((rows, rows), 0), iota((rows, rows), 1)
        acc_col = jnp.sum(jnp.where(a == b, row_acc[...], 0.0), axis=1, keepdims=True)
        new_col = DECAY * acc_col + (1.0 - DECAY) * (sums[0] / s.c)
        row_new[...] = jnp.sum(jnp.where(a == b, new_col, 0.0), axis=0, keepdims=True)
        scales[:, 4:5] = new_col

    group = (f * (s.rep * rows)).astype(F32)
    which = fiota((8, 1), 0)
    first, last, _ = ranges(jnp.where(which == 0.0, group + (s.rep * rows - 1), group), start, end)
    coef = []
    for k in range(s.rep):
        at = group + (rem(r + s.rep - k, s.rep) * rows).astype(F32)
        head = jnp.where((at >= first) & (at < last), 1.0, 0.0)
        tail = jnp.where((at + (rows - 1) >= first) & (at + (rows - 1) < last), 1.0, 0.0)
        coef.append((head, tail * (1.0 - head)))

    width, m, taps = (FIN + 4) * s.hm, 8 * s.hm, 8 * (FIN + 2)
    lw = iota((m, width), 1)
    spread = jnp.where(rem(iota((m, 8), 0), 8) == iota((m, 8), 1), 1.0, 0.0).astype(BF16)
    keep = (rem(lw, s.hm) == div(iota((m, width), 0), 8)) & (lw < (FIN + 1) * s.hm)
    fold = jnp.where(div(iota((width, taps), 0), s.hm) == div(iota((width, taps), 1), 8), 1.0, 0.0).astype(BF16)
    diag1 = (rem(iota((m, taps), 0), 8) == rem(iota((m, taps), 1), 8)) & (iota((m, taps), 1) < 8 * (FIN + 1))
    diag2 = iota((8, m), 0) == rem(iota((8, m), 1), 8)
    for o in range(3):
        want = (FIN + 1) * s.hm + 3 * div(iota((width, m), 1), 8) + o
        pick_w2[o] = jnp.where(iota((width, m), 0) == want, 1.0, 0.0).astype(BF16)

    with jax.named_scope("wait_p"):
        then = {6: (0,), 5: (1, 7), 4: (2, 6)} if ring else {}
        for k in near:
            c_p[k].wait_recv()
            pass_on(k, table.at[core, 0, k])
            for piece in then.get(k, ()):
                relay(piece)
        c_d = [remote(table.at[core, k], table.at[core, k], sent.at[d_k], one_come.at[d_k], f, partner) for k in range(s.nz)]
        c_d[0].start()
    with jax.named_scope("wait_g"):
        a, b = iota((nt, nt), 0), iota((nt, nt), 1)
        k1, p2, j2 = div(a, per), rem(div(a, 2), s.nz), rem(a, 2)
        slot = (1 - core) * (p2 * per + rem(y + k1, s.ny) * 2 + j2) + core * (rem(z + k1, s.nz) * per + p2 * 2 + j2)
        order_col = jnp.sum(jnp.where(b == slot, order, 0.0), axis=1, keepdims=True)
        ids = b.astype(F32)
        end_col = jnp.sum(jnp.where(ids <= order_col, lens, 0.0), axis=1, keepdims=True)
        start_col = end_col - jnp.sum(jnp.where(ids == order_col, lens, 0.0), axis=1, keepdims=True)
        all_come(gx.at[pl.ds(1, s.rep - 1)], g_k, f, r)
        part = jnp.zeros((nt, s.sl), F32)
        for k in range(s.rep):
            at = group + (rem(r + s.rep - k, s.rep) * rows).astype(F32) + fiota((1, rows), 1)
            part = part + jnp.dot(slot_hits(at, start_col, end_col).astype(BF16), gx[k], preferred_element_type=F32)
        for k in range(s.nz):
            zsrc[k] = part[k * per : (k + 1) * per].astype(BF16)
        c_z = [remote(zsrc.at[k], zbuf.at[k], sent.at[z_k], one_come.at[z_k], first_axis(k), r) for k in zs]
        for c in c_z:
            c.start()
        zbuf[0] = zsrc[0]
    with jax.named_scope("wait_ht"):
        all_come(htall.at[pl.ds(1, s.rep - 1)], ht_k, f, r)
        acc = jnp.zeros((2, s.cw), F32)
        for k in range(s.rep):
            both = htall[k].astype(F32)
            acc = acc + coef[k][0][:2] * both[0:1] + coef[k][1][:2] * both[1:2]
            ht16[2 * k : 2 * k + 2, :] = both
        acc = jnp.concatenate([acc[:, : s.c], restack(acc[:, s.c :])], axis=1)
        nbsrc[0] = jnp.broadcast_to(acc[0:1], (2, s.cw)).astype(BF16)
        nbsrc[1] = jnp.broadcast_to(acc[1:2], (2, s.cw)).astype(BF16)
        c_nb = [remote(nbsrc.at[i], nb.at[i], sent.at[nb_k], one_come.at[nb_k + 4 + i], to, r) for i, to in enumerate((nxt, prv))]
        for c in c_nb:
            c.start()

    n = s.all_rows
    row = iota((n, 1), 0)
    pos = jnp.where(row < rows, base + row.astype(F32), -1.0)
    lane = iota((n, nt), 1)
    hits = slot_hits(pos, start, end)
    hits = hits + jnp.where((row >= rows) & (row < rows + 2) & (lane == row - rows + 2 * f), 1.0, 0.0)
    first = jnp.sum(hits * start, axis=1, keepdims=True)
    last = jnp.sum(hits * end, axis=1, keepdims=True)
    length = jnp.maximum(last - first, 1.0)
    slot_of = jnp.sum(hits * lane.astype(F32), axis=1, keepdims=True)[:rows]
    first, last = first[:rows], last[:rows]
    same = slot_hits(base + fiota((1, rows), 1), first, last).astype(BF16)
    la = iota((1, 2 * s.rep), 1)
    head = group + (rem(r + s.rep - div(la, 2), s.rep) * rows).astype(F32)
    in_head = slot_hits(head, first, last)
    in_tail = slot_hits(head + (rows - 1), first, last) * (1.0 - in_head)
    shared = jnp.where(div(la, 2) == 0, 0.0, jnp.where(rem(la, 2) == 0, in_head, in_tail)).astype(BF16)
    before = slot_hits(group - 1.0, first, last)
    after = slot_hits(group + s.rep * rows, first, last)
    deep = s.nz * s.ny * 8
    lane = iota((rows, deep), 1)
    k2, k1, q4, j2 = div(lane, 8 * s.ny), rem(div(lane, 8), s.ny), rem(div(lane, 2), 4), rem(lane, 2)
    picks = []
    for half in range(2):
        kz, ky = (k2, k1) if half == 0 else (k1, k2)
        slot = rem(z + s.nz - kz, s.nz) * per + rem(y + s.ny - ky, s.ny) * 2 + j2
        hit = slot.astype(F32) == slot_of
        picks.append(jnp.concatenate([jnp.where(hit & (q4 == q), 1.0, 0.0) for q in range(4)], axis=0).astype(BF16))
    top = iota((8, 1), 0)

    def own_rows(v):
        return jnp.where(top == 0, v[0:1], jnp.where(top == 1, v[1:2], 0.0))

    def full_sums(g, lo, hi):
        out = jnp.dot(same, g, preferred_element_type=F32)
        out = out + jnp.dot(shared, ht16[:, lo:hi].astype(BF16), preferred_element_type=F32)
        return out + before * nb[0, :, lo:hi].astype(F32)[0:1] + after * nb[1, :, lo:hi].astype(F32)[0:1]

    with jax.named_scope("wait_t"):
        for k in near:
            ref = table.at[core, k, pl.ds(3, 3)] if ring and k in (2, 6) else table.at[core, k]
            remote(ref, ref, sent.at[t_k], t_come.at[k], f, r).wait_recv()
            c_d[k].start()
    with jax.named_scope("wait_z"):
        all_come(zbuf.at[pl.ds(1, s.nz - 1)], z_k, f, r)
        total = zbuf[0].astype(F32)
        for k in zs:
            total = total + zbuf[k].astype(F32)
        total = total.astype(BF16)
        for k in range(s.ny):
            ysrc[k] = total[2 * k : 2 * k + 2]
        second = (1 - core) * z + core * y
        c_y = []
        for a in range(s.ny):
            for b in range(s.rep):
                if a or b:
                    c_y.append(remote(ysrc.at[rem(second + a, s.ny)], ybuf.at[a, r], sent.at[y_k if a else y0_k],
                                      y_come.at[a if a else s.ny + b], second_axis(a), at_rep(b)))
        for c in c_y:
            c.start()
        ybuf[0, r] = ysrc[second]

    with jax.named_scope("wait_d"):
        for c in c_nb:
            c.wait_recv()
        all_come(table.at[1 - core], d_k, f, partner)

    with jax.named_scope("rows"):
        for half in range(2):
            got = jnp.dot(picks[half], table[half].reshape(deep, s.q), preferred_element_type=F32)
            for q in range(4):
                held[:, (4 * half + q) * s.q : (4 * half + q + 1) * s.q] = got[q * rows : (q + 1) * rows]
        total_col = jnp.zeros((rows, 1), F32)
        total_sq = jnp.zeros((rows, 1), F32)
        size = length[:rows]
        for j in range(chunks):
            lo, hi = j * s.sl, (j + 1) * s.sl
            new = DECAY * held[:, lo:hi] + (1.0 - DECAY) * full_sums(gs[j], lo, hi) / size
            cols[:, lo:hi] = new
            total_col = total_col + jnp.sum(new, axis=1, keepdims=True)
            total_sq = total_sq + jnp.sum(new * new, axis=1, keepdims=True)
        stats = full_sums(gs[chunks, :, :128], s.c, s.cw)
        means = [(stats[:, k : k + 1] + stats[:, k + 8 : k + 9]) / (size * s.c) for k in range(8)]
        col_mean = total_col / s.c
        feats = log_features(means, col_mean, total_sq / s.c)
        for c in weights:
            c.wait()
        hid = jnp.concatenate([held[:, s.c : s.c + s.hid], own_rows(hidden[...])], axis=0).astype(BF16)
        old = held[:, s.c + s.hid : s.c + 2 * s.hid] + held[:, s.c + 2 * s.hid : s.c + 3 * s.hid]

        def rec(k):
            out = jnp.dot(hid, w_rec[:, k * s.hid : (k + 1) * s.hid], preferred_element_type=F32)
            own_rec[k] = out[rows:]
            return out[:rows]

        state, _ = cell_step(s, feats, rec, w_in, bias, old)
        bf = state.astype(BF16)
        gen[:, : FIN * s.hm] = jnp.dot(bf, w_first[...], preferred_element_type=F32)
        gen[:, FIN * s.hm :] = jnp.dot(bf, w_rest[...], preferred_element_type=F32)
        scales[:, 0:1] = scales[:, 4:5] / col_mean
        for i, k in enumerate((0, 1, 4)):
            scales[:, i + 1 : i + 2] = 1.0 / jnp.sqrt(means[k] + EPS)

    wide = s.c // 2 if s.c % 256 == 0 else s.c
    ones, zeros = jnp.ones((8, wide), F32), jnp.zeros((8, wide), F32)

    blocks = rows // 16
    outs = []

    def block(i):
        at = 16 * i
        made = gen[at : at + 16, :].astype(BF16).astype(F32)
        sc = scales[at : at + 16, :]
        nets = []
        for half in range(2):
            mine = made[8 * half : 8 * half + 8].astype(BF16)
            y1 = jnp.where(keep, jnp.dot(spread, mine, preferred_element_type=F32), 0.0).astype(BF16)
            w1 = jnp.where(diag1, jnp.dot(y1, fold, preferred_element_type=F32), 0.0).astype(BF16)
            w2 = [jnp.where(diag2, jnp.dot(mine, pick_w2[o], preferred_element_type=F32), 0.0) for o in range(3)]
            nets.append((w1, jnp.concatenate(w2, axis=0).astype(BF16)))
        for j in range(s.c // wide):
            lo, hi = j * wide, (j + 1) * wide
            g16 = grads[at : at + 16, lo:hi].astype(F32)
            m16 = [moments[k, at : at + 16, lo:hi].astype(F32) for k in range(3)]
            p16 = params[at : at + 16, lo:hi]
            c16 = cols[at : at + 16, lo:hi]
            for half in range(2):
                q = slice(8 * half, 8 * half + 8)
                g, m0, m1, m2, p, cn = g16[q], m16[0][q], m16[1][q], m16[2][q], p16[q], c16[q]
                rms = lax.rsqrt(cn * sc[q, 0:1] + EPS)
                gn, mn = g * rms, m0 * rms
                x = jnp.concatenate(
                    [gn, mn, m1 * rms, m2 * rms, g * sc[q, 1:2], m0 * sc[q, 2:3], p * sc[q, 3:4], gn * mn, ones, zeros],
                    axis=0,
                ).astype(BF16)
                w1, w2 = nets[half]
                unit = jnp.maximum(jnp.dot(w1, x, preferred_element_type=F32), 0.0).astype(BF16)
                o = jnp.dot(w2, unit, preferred_element_type=F32)
                out = o[0:8] * jnp.exp(jnp.tanh(o[8:16])) * jax.nn.sigmoid(o[16:24])
                update[at + 8 * half : at + 8 * half + 8, lo:hi] = out

        c = pltpu.make_async_copy(update.at[pl.ds(at, 16)], update_h.at[pl.ds(at, 16)], s_out.at[i])
        c.start()
        outs.append(c)

    def owners():
        for a in ys:
            remote(ybuf.at[a], ybuf.at[a], sent.at[y_k], y_come.at[a], f, r).wait_recv()
        for c in c_y[: s.rep - 1]:
            c.wait_recv()
        size = length[rows:]

        def arrived(j):
            t = ybuf[0, j].astype(F32)
            for a in range(1, s.ny):
                t = t + ybuf[a, j].astype(F32)
            return own_rows(t)

        total_col = jnp.zeros((8, 1), F32)
        total_sq = jnp.zeros((8, 1), F32)
        for j in range(chunks):
            lo, hi = j * s.sl, (j + 1) * s.sl
            new = DECAY * own_rows(col_acc[:, lo:hi]) + (1.0 - DECAY) * arrived(j) / size
            col_new[:, lo:hi] = new[:2]
            total_col = total_col + jnp.sum(new, axis=1, keepdims=True)
            total_sq = total_sq + jnp.sum(new * new, axis=1, keepdims=True)
        stats = arrived(chunks)[:, :128]
        means = [(stats[:, k : k + 1] + stats[:, k + 8 : k + 9]) / (size * s.c) for k in range(8)]
        feats = log_features(means, total_col / s.c, total_sq / s.c)
        state, now = cell_step(s, feats, lambda k: own_rec[k], w_in, bias, own_rows(cell[...]))
        hidden_new[...] = state[:2]
        cell_new[...] = now[:2]
        for i, (a, b) in enumerate(((row_new, row_new_h), (col_new, col_new_h), (hidden_new, hidden_new_h), (cell_new, cell_new_h))):
            c = pltpu.make_async_copy(a, b, s_out.at[blocks + i])
            c.start()
            outs.append(c)

    for i in range(blocks):
        with jax.named_scope("block"):
            block(i)
    with jax.named_scope("owners"):
        owners()
    with jax.named_scope("drain"):
        def all_sent(ref, kind):
            remote(ref, ref, sent.at[kind], one_come.at[kind], f, r).wait_send()

        some, others = pl.ds(1, s.rep - 1), pl.ds(1, s.nz - 1)
        all_sent(htall.at[some], ht_k)
        all_sent(gx.at[some], g_k)
        all_sent(zbuf.at[others], z_k)
        all_sent(table.at[core], d_k)
        all_sent(nb, nb_k)
        all_sent(table.at[core, 0, others], p_k)
        all_sent(table.at[core, others], t_k)
        all_sent(ybuf.at[others], y_k)
        all_sent(ybuf.at[0, some], y0_k)
        for c in outs:
            c.wait()


def put_out(*refs):
    here, there, held, sems = refs[:5], refs[5:10], refs[10:15], refs[15]
    come = [pltpu.make_async_copy(a, b, sems.at[0, i]) for i, (a, b) in enumerate(zip(here, held))]
    go = [pltpu.make_async_copy(a, b, sems.at[1, i]) for i, (a, b) in enumerate(zip(held, there))]
    for c in come:
        c.start()
    for a, b in zip(come, go):
        a.wait()
        b.start()
    for c in go:
        c.wait()


def on_device(s, params, grads, moments, row_acc, lengths, tensor_order, col_acc, hidden_state, cell_state,
              lstm_in, lstm_rec, lstm_bias, hyper_first, hyper_rest):
    shape = jax.ShapeDtypeStruct
    rows, per, width = s.rows, 2 * s.ny, (FIN + 4) * s.hm
    args = (params, grads, moments, row_acc.reshape(1, rows), lengths.reshape(1, s.nt), tensor_order.reshape(1, s.nt),
            col_acc, hidden_state, cell_state, lstm_in, lstm_rec, lstm_bias.reshape(1, -1), hyper_first, hyper_rest)

    def sems(k):
        return pltpu.SemaphoreType.DMA((2, k))

    def one(k):
        return pltpu.SemaphoreType.DMA((k,))

    outs = (
        shape(params.shape, F32), shape((1, rows), F32), shape(col_acc.shape, F32), shape(hidden_state.shape, F32),
        shape(cell_state.shape, F32),
    )
    made = pl.pallas_call(
        functools.partial(kernel, s),
        out_shape=outs,
        in_specs=[ANY] * len(args),
        out_specs=(ANY,) * 5,
        scratch_shapes=[VMEM(a.shape, a.dtype) for a in args] + [
            one(6), one(5), one(5), one(rows // 16 + 4),
            VMEM((s.rep, rows, s.sl), BF16), VMEM((2, s.cw), BF16), VMEM((2, 8, s.q), BF16),
            VMEM((s.rep, 2, s.cw), BF16), VMEM((2, 2, s.cw), BF16), VMEM((2, s.nz, s.ny, 8, s.q), BF16),
            VMEM((2, 2, s.cw), BF16), VMEM((s.rep, rows, s.sl), BF16),
            VMEM((s.nz, per, s.sl), BF16), VMEM((s.nz, per, s.sl), BF16), VMEM((s.ny, 2, s.sl), BF16),
            VMEM((s.ny, s.rep, 2, s.sl), BF16),
            one(9), one(10), one(s.ny), one(8 + 2 * s.ny), one(s.ny + s.rep),
            VMEM((rows, s.c), F32), VMEM((2 * s.rep, s.cw), F32), VMEM((rows, width), F32), VMEM((rows, 128), F32),
            VMEM((3, width, 8 * s.hm), BF16), VMEM((4, 8, s.hid), F32),
            VMEM((rows, 8 * s.q), F32),
        ] + [VMEM(o.shape, o.dtype) for o in outs],
        compiler_params=pltpu.CompilerParams(collective_id=0, has_side_effects=True, vmem_limit_bytes=LIMIT),
        name="step",
    )(*args)
    update, row_new, col_new, hidden_new, cell_new = pl.pallas_call(
        put_out,
        out_shape=outs,
        in_specs=[ANY] * 5,
        out_specs=(ANY,) * 5,
        scratch_shapes=[VMEM(o.shape, o.dtype) for o in outs] + [sems(5)],
        compiler_params=pltpu.CompilerParams(vmem_limit_bytes=LIMIT),
        name="out",
    )(*made)
    return update, row_new.reshape(rows), col_new, hidden_new, cell_new


def solution(mesh):
    rowwise, owned, everywhere = P(("fsdp", "rep"), None), P("fsdp", None), P()

    def step(params, grads, moments, row_acc, lengths, tensor_order, col_acc, hidden_state, cell_state, *weights):
        s = Sizes(mesh, params, col_acc, hidden_state, weights[-1])
        return jax.shard_map(
            functools.partial(on_device, s),
            mesh=mesh,
            in_specs=(rowwise, rowwise, P(None, ("fsdp", "rep"), None), P(("fsdp", "rep")), everywhere, everywhere,
                      owned, owned, owned) + (everywhere,) * 5,
            out_specs=(rowwise, P(("fsdp", "rep")), owned, owned, owned),
            check_vma=False,
        )(params, grads, moments, row_acc, lengths, tensor_order, col_acc, hidden_state, cell_state, *weights)

    return step
```

```python
import functools
import math

import jax
import jax.numpy as jnp
from jax import lax
from jax.experimental import pallas as pl
from jax.experimental.pallas import tpu as pltpu
from jax.sharding import PartitionSpec as P

EPS = 1e-06
DECAY = 0.9
FIN = 8
F32 = jnp.float32
BF16 = jnp.bfloat16
MESH = pl.DeviceIdType.MESH
VMEM = pltpu.VMEM
LIMIT = 60 * 1024 * 1024
ANY = pl.BlockSpec(memory_space=pltpu.HBM)


class Sizes:
    def __init__(self, mesh, params, col_acc, hidden_state, rest):
        self.fsdp, self.rep = mesh.shape["fsdp"], mesh.shape["rep"]
        self.nz = self.ny = math.isqrt(self.fsdp)
        self.nt = col_acc.shape[0]
        self.own = self.nt // self.fsdp
        self.rows = params.shape[0] // (self.fsdp * self.rep)
        self.c = params.shape[1]
        self.hid = hidden_state.shape[1]
        self.hm = rest.shape[1] // 4
        self.sl = self.c // (self.rep - 1)
        self.cw = self.c + 128
        self.q = -(-(self.c + 3 * self.hid) // 1024) * 128
        self.all_rows = self.rows + 8
        assert self.own == 2 and self.sl % 128 == 0 and self.rows % 16 == 0


def iota(shape, dim):
    return lax.broadcasted_iota(jnp.int32, shape, dim)


def fiota(shape, dim):
    return iota(shape, dim).astype(F32)


def rem(a, b):
    return lax.rem(a, jnp.int32(b))


def div(a, b):
    return lax.div(a, jnp.int32(b))


def slot_bounds(s, lens, order):
    a, b = iota((s.nt, s.nt), 0), iota((s.nt, s.nt), 1)
    lens_col = jnp.sum(jnp.where(a == b, lens, 0.0), axis=1, keepdims=True)
    ids = a.astype(F32)
    end = jnp.sum(jnp.where(ids <= order, lens_col, 0.0), axis=0, keepdims=True)
    size = jnp.sum(jnp.where(ids == order, lens_col, 0.0), axis=0, keepdims=True)
    return end - size, end


def slot_hits(pos, start, end):
    return jnp.where((pos >= start) & (pos < end), 1.0, 0.0)


def ranges(pos, start, end):
    hits = slot_hits(pos, start, end)
    first = jnp.sum(hits * start, axis=1, keepdims=True)
    last = jnp.sum(hits * end, axis=1, keepdims=True)
    return first, last, hits


def split2(x):
    hi = x.astype(BF16)
    return hi, (x - hi.astype(F32)).astype(BF16)


def restack(t):
    lane = iota(t.shape, 1)
    both = t + pltpu.roll(t, 120, 1)
    hi = both.astype(BF16).astype(F32)
    low = pltpu.roll(both - hi, 8, 1)
    return jnp.where(lane < 8, hi, jnp.where(lane < 16, low, 0.0))


def remote(src, dst, send_sem, recv_sem, fsdp, rep):
    return pltpu.make_async_remote_copy(
        src_ref=src, dst_ref=dst, send_sem=send_sem, recv_sem=recv_sem,
        device_id={"fsdp": fsdp, "rep": rep}, device_id_type=MESH,
    )


def log_features(means, col_mean, col_square):
    feats = [jnp.log(means[k] + EPS) for k in range(5)]
    feats += [means[5] / jnp.sqrt(means[0] * means[1] + EPS), means[6] / jnp.sqrt(means[0] * means[3] + EPS),
              means[7] / jnp.sqrt(means[1] * means[3] + EPS), jnp.log(col_mean + EPS),
              jnp.log(col_square / (col_mean * col_mean))]
    return [v.astype(BF16).astype(F32) for v in feats]


def cell_step(s, feats, rec, w_in, bias, old):
    def gate(k):
        lo, hi = k * s.hid, (k + 1) * s.hid
        out = rec(k) + bias[:, lo:hi]
        w = w_in[:, lo:hi].astype(F32)
        for i, v in enumerate(feats):
            out = out + v * w[i : i + 1]
        return out

    now = jax.nn.sigmoid(gate(1)) * old + jax.nn.sigmoid(gate(0)) * jnp.tanh(gate(2))
    return jax.nn.sigmoid(gate(3)) * jnp.tanh(now), now


def kernel(s, params_h, grads_h, moments_h, row_acc_h, lens_h, order_h, col_acc_h, hidden_h, cell_h, w_in_h, w_rec_h,
           bias_h, w_first_h, w_rest_h,
           update_h, row_new_h, col_new_h, hidden_new_h, cell_new_h,
           params, grads, moments, row_acc, lens_i, order_i, col_acc, hidden, cell, w_in, w_rec, bias, w_first, w_rest,
           s_in, s_big, s_w, s_out,
           gs, ht, ag, htall, nb, table, nbsrc, gx, zsrc, zbuf, ysrc, ybuf,
           sent, one_come, p_come, t_come, y_come,
           cols, ht16, gen, scales, pick_w2, net1, net2, own_rec, held, update, row_new, col_new, hidden_new, cell_new):
    f, r = lax.axis_index("fsdp"), lax.axis_index("rep")
    z, y, core = div(f, s.ny), rem(f, s.ny), rem(r, 2)
    partner = r + 1 - 2 * core
    nxt, prv = rem(f + 1, s.fsdp), rem(f + s.fsdp - 1, s.fsdp)
    rows, nt, chunks, per = s.rows, s.nt, s.rep - 1, 2 * s.ny
    reps, ys, zs = range(1, s.rep), range(1, s.ny), range(1, s.nz)

    def at_rep(k):
        return rem(r + k, s.rep)

    def at_y(k):
        return z * s.ny + rem(y + k, s.ny)

    def at_z(k):
        return rem(z + k, s.nz) * s.ny + y

    ht_k, g_k, z_k, d_k, nb_k, p_k, t_k, y_k, y0_k = range(9)

    def all_come(ref, kind, fsdp, rep):
        remote(ref, ref, sent.at[kind], one_come.at[kind], fsdp, rep).wait_recv()

    def first_axis(k):
        return (1 - core) * at_y(k) + core * at_z(k)

    def second_axis(k):
        return (1 - core) * at_z(k) + core * at_y(k)

    with jax.named_scope("greet"):
        def fetch(pairs, sem):
            made = [pltpu.make_async_copy(a, b, sem.at[i]) for i, (a, b) in enumerate(pairs)]
            for c in made:
                c.start()
            return made

        small = fetch([(col_acc_h, col_acc), (hidden_h, hidden), (cell_h, cell), (lens_h, lens_i), (order_h, order_i),
                       (row_acc_h, row_acc)], s_in)
        big = fetch([(grads_h, grads)] + [(moments_h.at[k], moments.at[k]) for k in range(3)] + [(params_h, params)], s_big)
        barrier = pltpu.get_barrier_semaphore()
        peers = [(at_z(k), 2 * x) for k in zs for x in range(s.rep // 2)]
        peers += [(at_y(k), 2 * x + 1) for k in ys for x in range(s.rep // 2)]
        peers += [(f, at_rep(k)) for k in reps] + [(first_axis(k), r) for k in ys] + [(nxt, r), (prv, r)]
        for pf, pr in peers:
            pl.semaphore_signal(barrier, inc=1, device_id={"fsdp": pf, "rep": pr}, device_id_type=MESH)
    def fetch_weights():
        return fetch([(w_rec_h, w_rec), (w_in_h, w_in), (bias_h, bias), (w_first_h, w_first), (w_rest_h, w_rest)], s_w)

    with jax.named_scope("own"):
        for c in small[:3]:
            c.wait()
        own = jnp.concatenate([v.astype(BF16) for v in (col_acc[...], hidden[...])] + list(split2(cell[...])), axis=1)
        if s.c + 3 * s.hid < 8 * s.q:
            own = jnp.concatenate([own, jnp.zeros((2, 8 * s.q - s.c - 3 * s.hid), BF16)], axis=1)
        own = own.astype(F32)
        for half in range(2):
            parts = [own[:, (4 * half + q) * s.q : (4 * half + q + 1) * s.q] for q in range(4)]
            ag[half] = jnp.concatenate(parts, axis=0).astype(BF16)
    with jax.named_scope("meet"):
        pl.semaphore_wait(barrier, len(peers))
        c_p = {k: remote(ag.at[core], table.at[core, 0, k], sent.at[p_k], p_come.at[k], first_axis(k), r) for k in ys}
        near = sorted(zs, key=lambda k: min(k, s.nz - k))
        ring = s.nz == 8
        early = (0, 1, 7, 2, 6) if ring else ()
        t_two = {}

        def hop(src, slot, piece, to):
            sem = t_come.at[8 + 2 * piece + (slot == 6)] if slot in (2, 6) and piece in early else t_come.at[slot]
            c = remote(src, table.at[core, slot, piece], sent.at[t_k], sem, second_axis(to), r)
            c.start()
            return c

        def pass_on(piece, src):
            for k in (2, 6, 1, 7) if piece in early else near[::-1]:
                t_two[k, piece] = hop(src, k, piece, k)

        def relay(piece):
            t_two[2, piece].wait_recv()
            if piece % 2 == 0:
                hop(table.at[core, 2, piece], 4, piece, 2)
            hop(table.at[core, 2, piece], 3, piece, 1)
            t_two[6, piece].wait_recv()
            if piece % 2 == 1:
                hop(table.at[core, 6, piece], 4, piece, 6)
            hop(table.at[core, 6, piece], 5, piece, 7)

        for k in near[::-1]:
            c_p[k].start()
        pass_on(0, ag.at[core])
        table[core, 0, 0] = ag[core]

    with jax.named_scope("stats"):
        for c in big:
            c.wait()
        sums = [jnp.zeros((rows, 1), F32) for _ in range(8)]
        for j in range(chunks):
            cs = pl.ds(j * s.sl, s.sl)
            g, p = grads[:, cs].astype(F32), params[:, cs]
            m = [moments[k, :, cs].astype(F32) for k in range(3)]
            sq = g * g
            gs[j] = sq.astype(BF16)
            for k, v in enumerate((sq, m[0] * m[0], m[1] * m[1], m[2] * m[2], p * p, g * m[0], g * m[2], m[0] * m[2])):
                sums[k] = sums[k] + jnp.sum(v, axis=1, keepdims=True)
        lane = iota((rows, 128), 1)
        stats = jnp.zeros((rows, 128), F32)
        for k in range(8):
            hi, low = split2(sums[k])
            stats = jnp.where(lane == k, hi.astype(F32), stats)
            stats = jnp.where(lane == k + 8, low.astype(F32), stats)
        gs[chunks] = jnp.zeros((rows, s.sl), BF16)
        gs[chunks, :, :128] = stats.astype(BF16)
    with jax.named_scope("send1"):
        c_g = [remote(gs.at[at_rep(k)], gx.at[k], sent.at[g_k], one_come.at[g_k], f, at_rep(k)) for k in reps]
        for c in c_g:
            c.start()
        weights = fetch_weights()
    with jax.named_scope("ends"):
        for c in small[3:]:
            c.wait()
        lens, order = lens_i[...].astype(F32), order_i[...].astype(F32)
        start, end = slot_bounds(s, lens, order)
        base = ((f * s.rep + r) * rows).astype(F32)
        which = fiota((16, 1), 0)
        pos = jnp.where(which == 0.0, base, jnp.where(which == 1.0, base + (rows - 1), -1.0))
        first, last, _ = ranges(pos, start, end)
        here = base + fiota((1, rows), 1)
        pick = slot_hits(here, first, last).astype(BF16)
        for j in range(chunks):
            part = jnp.dot(pick, gs[j], preferred_element_type=F32)
            ht[:, j * s.sl : (j + 1) * s.sl] = part[:2].astype(BF16)
        part = jnp.dot(pick, gs[chunks, :, :128], preferred_element_type=F32)
        ht[:, s.c :] = restack(part)[:2].astype(BF16)
        c_ht = [remote(ht, htall.at[k], sent.at[ht_k], one_come.at[ht_k], f, at_rep(k)) for k in reps]
        for c in c_ht:
            c.start()
        htall[0] = ht[...]
        gx[0] = gs[r]
        a, b = iota((rows, rows), 0), iota((rows, rows), 1)
        acc_col = jnp.sum(jnp.where(a == b, row_acc[...], 0.0), axis=1, keepdims=True)
        new_col = DECAY * acc_col + (1.0 - DECAY) * (sums[0] / s.c)
        row_new[...] = jnp.sum(jnp.where(a == b, new_col, 0.0), axis=0, keepdims=True)
        scales[:, 4:5] = new_col

    group = (f * (s.rep * rows)).astype(F32)
    which = fiota((8, 1), 0)
    first, last, _ = ranges(jnp.where(which == 0.0, group + (s.rep * rows - 1), group), start, end)
    coef = []
    for k in range(s.rep):
        at = group + (rem(r + s.rep - k, s.rep) * rows).astype(F32)
        head = jnp.where((at >= first) & (at < last), 1.0, 0.0)
        tail = jnp.where((at + (rows - 1) >= first) & (at + (rows - 1) < last), 1.0, 0.0)
        coef.append((head, tail * (1.0 - head)))

    width, m, taps = (FIN + 4) * s.hm, 8 * s.hm, 8 * (FIN + 2)
    lw = iota((m, width), 1)
    spread = jnp.where(rem(iota((m, 8), 0), 8) == iota((m, 8), 1), 1.0, 0.0).astype(BF16)
    keep = (rem(lw, s.hm) == div(iota((m, width), 0), 8)) & (lw < (FIN + 1) * s.hm)
    fold = jnp.where(div(iota((width, taps), 0), s.hm) == div(iota((width, taps), 1), 8), 1.0, 0.0).astype(BF16)
    diag1 = (rem(iota((m, taps), 0), 8) == rem(iota((m, taps), 1), 8)) & (iota((m, taps), 1) < 8 * (FIN + 1))
    diag2 = iota((8, m), 0) == rem(iota((8, m), 1), 8)
    for o in range(3):
        want = (FIN + 1) * s.hm + 3 * div(iota((width, m), 1), 8) + o
        pick_w2[o] = jnp.where(iota((width, m), 0) == want, 1.0, 0.0).astype(BF16)

    with jax.named_scope("wait_p"):
        then = {6: (0,)} if ring else {}
        for k in near:
            c_p[k].wait_recv()
            pass_on(k, table.at[core, 0, k])
            for piece in then.get(k, ()):
                relay(piece)
    with jax.named_scope("wait_g"):
        a, b = iota((nt, nt), 0), iota((nt, nt), 1)
        k1, p2, j2 = div(a, per), rem(div(a, 2), s.nz), rem(a, 2)
        slot = (1 - core) * (p2 * per + rem(y + k1, s.ny) * 2 + j2) + core * (rem(z + k1, s.nz) * per + p2 * 2 + j2)
        order_col = jnp.sum(jnp.where(b == slot, order, 0.0), axis=1, keepdims=True)
        ids = b.astype(F32)
        end_col = jnp.sum(jnp.where(ids <= order_col, lens, 0.0), axis=1, keepdims=True)
        start_col = end_col - jnp.sum(jnp.where(ids == order_col, lens, 0.0), axis=1, keepdims=True)
        all_come(gx.at[pl.ds(1, s.rep - 1)], g_k, f, r)
        part = jnp.zeros((nt, s.sl), F32)
        for k in range(s.rep):
            at = group + (rem(r + s.rep - k, s.rep) * rows).astype(F32) + fiota((1, rows), 1)
            part = part + jnp.dot(slot_hits(at, start_col, end_col).astype(BF16), gx[k], preferred_element_type=F32)
        for k in range(s.nz):
            zsrc[k] = part[k * per : (k + 1) * per].astype(BF16)
        c_z = [remote(zsrc.at[k], zbuf.at[k], sent.at[z_k], one_come.at[z_k], first_axis(k), r) for k in zs]
        for c in c_z:
            c.start()
        zbuf[0] = zsrc[0]
    with jax.named_scope("relay"):
        for piece in (1, 7, 2, 6) if ring else ():
            relay(piece)
        c_d = [remote(table.at[core, k], table.at[core, k], sent.at[d_k], one_come.at[d_k], f, partner) for k in range(s.nz)]
        c_d[0].start()
    with jax.named_scope("wait_ht"):
        all_come(htall.at[pl.ds(1, s.rep - 1)], ht_k, f, r)
        acc = jnp.zeros((2, s.cw), F32)
        for k in range(s.rep):
            both = htall[k].astype(F32)
            acc = acc + coef[k][0][:2] * both[0:1] + coef[k][1][:2] * both[1:2]
            ht16[2 * k : 2 * k + 2, :] = both
        acc = jnp.concatenate([acc[:, : s.c], restack(acc[:, s.c :])], axis=1)
        nbsrc[0] = jnp.broadcast_to(acc[0:1], (2, s.cw)).astype(BF16)
        nbsrc[1] = jnp.broadcast_to(acc[1:2], (2, s.cw)).astype(BF16)
        c_nb = [remote(nbsrc.at[i], nb.at[i], sent.at[nb_k], one_come.at[nb_k + 4 + i], to, r) for i, to in enumerate((nxt, prv))]
        for c in c_nb:
            c.start()

    n = s.all_rows
    row = iota((n, 1), 0)
    pos = jnp.where(row < rows, base + row.astype(F32), -1.0)
    lane = iota((n, nt), 1)
    hits = slot_hits(pos, start, end)
    hits = hits + jnp.where((row >= rows) & (row < rows + 2) & (lane == row - rows + 2 * f), 1.0, 0.0)
    first = jnp.sum(hits * start, axis=1, keepdims=True)
    last = jnp.sum(hits * end, axis=1, keepdims=True)
    length = jnp.maximum(last - first, 1.0)
    slot_of = jnp.sum(hits * lane.astype(F32), axis=1, keepdims=True)[:rows]
    first, last = first[:rows], last[:rows]
    same = slot_hits(base + fiota((1, rows), 1), first, last).astype(BF16)
    la = iota((1, 2 * s.rep), 1)
    head = group + (rem(r + s.rep - div(la, 2), s.rep) * rows).astype(F32)
    in_head = slot_hits(head, first, last)
    in_tail = slot_hits(head + (rows - 1), first, last) * (1.0 - in_head)
    shared = jnp.where(div(la, 2) == 0, 0.0, jnp.where(rem(la, 2) == 0, in_head, in_tail)).astype(BF16)
    before = slot_hits(group - 1.0, first, last)
    after = slot_hits(group + s.rep * rows, first, last)
    deep = s.nz * s.ny * 8
    lane = iota((rows, deep), 1)
    k2, k1, q4, j2 = div(lane, 8 * s.ny), rem(div(lane, 8), s.ny), rem(div(lane, 2), 4), rem(lane, 2)
    picks = []
    for half in range(2):
        kz, ky = (k2, k1) if half == 0 else (k1, k2)
        slot = rem(z + s.nz - kz, s.nz) * per + rem(y + s.ny - ky, s.ny) * 2 + j2
        hit = slot.astype(F32) == slot_of
        picks.append(jnp.concatenate([jnp.where(hit & (q4 == q), 1.0, 0.0) for q in range(4)], axis=0).astype(BF16))
    top = iota((8, 1), 0)

    def own_rows(v):
        return jnp.where(top == 0, v[0:1], jnp.where(top == 1, v[1:2], 0.0))

    def full_sums(g, lo, hi):
        out = jnp.dot(same, g, preferred_element_type=F32)
        out = out + jnp.dot(shared, ht16[:, lo:hi].astype(BF16), preferred_element_type=F32)
        return out + before * nb[0, :, lo:hi].astype(F32)[0:1] + after * nb[1, :, lo:hi].astype(F32)[0:1]

    def got_block(k):
        ref = table.at[core, k, pl.ds(3, 3)] if ring and k in (2, 6) else table.at[core, k]
        remote(ref, ref, sent.at[t_k], t_come.at[k], f, r).wait_recv()
        c_d[k].start()

    with jax.named_scope("wait_t"):
        for k in near:
            got_block(k)
    with jax.named_scope("wait_nb"):
        for c in c_nb:
            c.wait_recv()
        size = length[:rows]
        for j in range(chunks):
            lo, hi = j * s.sl, (j + 1) * s.sl
            cols[:, lo:hi] = full_sums(gs[j], lo, hi) * ((1.0 - DECAY) / size)
        stats = full_sums(gs[chunks, :, :128], s.c, s.cw)
        means = [(stats[:, k : k + 1] + stats[:, k + 8 : k + 9]) / (size * s.c) for k in range(8)]
    with jax.named_scope("wait_z"):
        all_come(zbuf.at[pl.ds(1, s.nz - 1)], z_k, f, r)
        total = zbuf[0].astype(F32)
        for k in zs:
            total = total + zbuf[k].astype(F32)
        total = total.astype(BF16)
        for k in range(s.ny):
            ysrc[k] = total[2 * k : 2 * k + 2]
        second = (1 - core) * z + core * y
        c_y = []
        for a in range(s.ny):
            for b in range(s.rep):
                if a or b:
                    c_y.append(remote(ysrc.at[rem(second + a, s.ny)], ybuf.at[a, r], sent.at[y_k if a else y0_k],
                                      y_come.at[a if a else s.ny + b], second_axis(a), at_rep(b)))
        for c in c_y:
            c.start()
        ybuf[0, r] = ysrc[second]

    with jax.named_scope("wait_d"):
        all_come(table.at[1 - core], d_k, f, partner)

    with jax.named_scope("rows"):
        for half in range(2):
            got = jnp.dot(picks[half], table[half].reshape(deep, s.q), preferred_element_type=F32)
            for q in range(4):
                held[:, (4 * half + q) * s.q : (4 * half + q + 1) * s.q] = got[q * rows : (q + 1) * rows]
        total_col = jnp.zeros((rows, 1), F32)
        total_sq = jnp.zeros((rows, 1), F32)
        for j in range(chunks):
            lo, hi = j * s.sl, (j + 1) * s.sl
            new = DECAY * held[:, lo:hi] + cols[:, lo:hi]
            cols[:, lo:hi] = new
            total_col = total_col + jnp.sum(new, axis=1, keepdims=True)
            total_sq = total_sq + jnp.sum(new * new, axis=1, keepdims=True)
        col_mean = total_col / s.c
        feats = log_features(means, col_mean, total_sq / s.c)
        for c in weights:
            c.wait()
        hid = jnp.concatenate([held[:, s.c : s.c + s.hid], own_rows(hidden[...])], axis=0).astype(BF16)
        old = held[:, s.c + s.hid : s.c + 2 * s.hid] + held[:, s.c + 2 * s.hid : s.c + 3 * s.hid]

        def rec(k):
            out = jnp.dot(hid, w_rec[:, k * s.hid : (k + 1) * s.hid], preferred_element_type=F32)
            own_rec[k] = out[rows:]
            return out[:rows]

        state, _ = cell_step(s, feats, rec, w_in, bias, old)
        bf = state.astype(BF16)
        gen[:, : FIN * s.hm] = jnp.dot(bf, w_first[...], preferred_element_type=F32)
        gen[:, FIN * s.hm :] = jnp.dot(bf, w_rest[...], preferred_element_type=F32)
        scales[:, 0:1] = scales[:, 4:5] / col_mean
        for i, k in enumerate((0, 1, 4)):
            scales[:, i + 1 : i + 2] = 1.0 / jnp.sqrt(means[k] + EPS)

    wide = s.c // 2 if s.c % 256 == 0 else s.c
    ones, zeros = jnp.ones((8, wide), F32), jnp.zeros((8, wide), F32)

    blocks = rows // 16
    outs = []

    with jax.named_scope("nets"):
        made = gen[...].astype(BF16).astype(F32)
        groups = [made[8 * i : 8 * i + 8].astype(BF16) for i in range(rows // 8)]
        wide1 = [jnp.where(keep, jnp.dot(spread, v, preferred_element_type=F32), 0.0).astype(BF16) for v in groups]
        for i, v in enumerate(wide1):
            net1[i] = jnp.where(diag1, jnp.dot(v, fold, preferred_element_type=F32), 0.0).astype(BF16)
        by_out = [jnp.dot(gen[...].astype(BF16), pick_w2[o], preferred_element_type=F32) for o in range(3)]
        for i in range(rows // 8):
            w2 = [jnp.where(diag2, v[8 * i : 8 * i + 8], 0.0) for v in by_out]
            net2[i] = jnp.concatenate(w2, axis=0).astype(BF16)

    def block(i):
        at = 16 * i
        sc = scales[at : at + 16, :]
        nets = [(net1[2 * i + half], net2[2 * i + half]) for half in range(2)]
        for j in range(s.c // wide):
            lo, hi = j * wide, (j + 1) * wide
            g16 = grads[at : at + 16, lo:hi].astype(F32)
            m16 = [moments[k, at : at + 16, lo:hi].astype(F32) for k in range(3)]
            p16 = params[at : at + 16, lo:hi]
            c16 = cols[at : at + 16, lo:hi]
            for half in range(2):
                q = slice(8 * half, 8 * half + 8)
                g, m0, m1, m2, p, cn = g16[q], m16[0][q], m16[1][q], m16[2][q], p16[q], c16[q]
                rms = lax.rsqrt(cn * sc[q, 0:1] + EPS)
                gn, mn = g * rms, m0 * rms
                x = jnp.concatenate(
                    [gn, mn, m1 * rms, m2 * rms, g * sc[q, 1:2], m0 * sc[q, 2:3], p * sc[q, 3:4], gn * mn, ones, zeros],
                    axis=0,
                ).astype(BF16)
                w1, w2 = nets[half]
                unit = jnp.maximum(jnp.dot(w1, x, preferred_element_type=F32), 0.0).astype(BF16)
                o = jnp.dot(w2, unit, preferred_element_type=F32)
                out = o[0:8] * jnp.exp(jnp.tanh(o[8:16])) * jax.nn.sigmoid(o[16:24])
                update[at + 8 * half : at + 8 * half + 8, lo:hi] = out

        c = pltpu.make_async_copy(update.at[pl.ds(at, 16)], update_h.at[pl.ds(at, 16)], s_out.at[i])
        c.start()
        outs.append(c)

    def owners():
        for a in ys:
            remote(ybuf.at[a], ybuf.at[a], sent.at[y_k], y_come.at[a], f, r).wait_recv()
        for c in c_y[: s.rep - 1]:
            c.wait_recv()
        size = length[rows:]

        def arrived(j):
            t = ybuf[0, j].astype(F32)
            for a in range(1, s.ny):
                t = t + ybuf[a, j].astype(F32)
            return own_rows(t)

        total_col = jnp.zeros((8, 1), F32)
        total_sq = jnp.zeros((8, 1), F32)
        for j in range(chunks):
            lo, hi = j * s.sl, (j + 1) * s.sl
            new = DECAY * own_rows(col_acc[:, lo:hi]) + (1.0 - DECAY) * arrived(j) / size
            col_new[:, lo:hi] = new[:2]
            total_col = total_col + jnp.sum(new, axis=1, keepdims=True)
            total_sq = total_sq + jnp.sum(new * new, axis=1, keepdims=True)
        stats = arrived(chunks)[:, :128]
        means = [(stats[:, k : k + 1] + stats[:, k + 8 : k + 9]) / (size * s.c) for k in range(8)]
        feats = log_features(means, total_col / s.c, total_sq / s.c)
        state, now = cell_step(s, feats, lambda k: own_rec[k], w_in, bias, own_rows(cell[...]))
        hidden_new[...] = state[:2]
        cell_new[...] = now[:2]
        for i, (a, b) in enumerate(((row_new, row_new_h), (col_new, col_new_h), (hidden_new, hidden_new_h), (cell_new, cell_new_h))):
            c = pltpu.make_async_copy(a, b, s_out.at[blocks + i])
            c.start()
            outs.append(c)

    for i in range(blocks):
        with jax.named_scope("block"):
            block(i)
    with jax.named_scope("owners"):
        owners()
    with jax.named_scope("drain"):
        def all_sent(ref, kind):
            remote(ref, ref, sent.at[kind], one_come.at[kind], f, r).wait_send()

        some, others = pl.ds(1, s.rep - 1), pl.ds(1, s.nz - 1)
        all_sent(htall.at[some], ht_k)
        all_sent(gx.at[some], g_k)
        all_sent(zbuf.at[others], z_k)
        all_sent(table.at[core], d_k)
        all_sent(nb, nb_k)
        all_sent(table.at[core, 0, others], p_k)
        all_sent(table.at[core, others], t_k)
        all_sent(ybuf.at[others], y_k)
        all_sent(ybuf.at[0, some], y0_k)
        for c in outs:
            c.wait()


def put_out(*refs):
    here, there, held, sems = refs[:5], refs[5:10], refs[10:15], refs[15]
    come = [pltpu.make_async_copy(a, b, sems.at[0, i]) for i, (a, b) in enumerate(zip(here, held))]
    go = [pltpu.make_async_copy(a, b, sems.at[1, i]) for i, (a, b) in enumerate(zip(held, there))]
    for c in come:
        c.start()
    for a, b in zip(come, go):
        a.wait()
        b.start()
    for c in go:
        c.wait()


def on_device(s, params, grads, moments, row_acc, lengths, tensor_order, col_acc, hidden_state, cell_state,
              lstm_in, lstm_rec, lstm_bias, hyper_first, hyper_rest):
    shape = jax.ShapeDtypeStruct
    rows, per, width = s.rows, 2 * s.ny, (FIN + 4) * s.hm
    args = (params, grads, moments, row_acc.reshape(1, rows), lengths.reshape(1, s.nt), tensor_order.reshape(1, s.nt),
            col_acc, hidden_state, cell_state, lstm_in, lstm_rec, lstm_bias.reshape(1, -1), hyper_first, hyper_rest)

    def sems(k):
        return pltpu.SemaphoreType.DMA((2, k))

    def one(k):
        return pltpu.SemaphoreType.DMA((k,))

    outs = (
        shape(params.shape, F32), shape((1, rows), F32), shape(col_acc.shape, F32), shape(hidden_state.shape, F32),
        shape(cell_state.shape, F32),
    )
    made = pl.pallas_call(
        functools.partial(kernel, s),
        out_shape=outs,
        in_specs=[ANY] * len(args),
        out_specs=(ANY,) * 5,
        scratch_shapes=[VMEM(a.shape, a.dtype) for a in args] + [
            one(6), one(5), one(5), one(rows // 16 + 4),
            VMEM((s.rep, rows, s.sl), BF16), VMEM((2, s.cw), BF16), VMEM((2, 8, s.q), BF16),
            VMEM((s.rep, 2, s.cw), BF16), VMEM((2, 2, s.cw), BF16), VMEM((2, s.nz, s.ny, 8, s.q), BF16),
            VMEM((2, 2, s.cw), BF16), VMEM((s.rep, rows, s.sl), BF16),
            VMEM((s.nz, per, s.sl), BF16), VMEM((s.nz, per, s.sl), BF16), VMEM((s.ny, 2, s.sl), BF16),
            VMEM((s.ny, s.rep, 2, s.sl), BF16),
            one(9), one(10), one(s.ny), one(8 + 2 * s.ny), one(s.ny + s.rep),
            VMEM((rows, s.c), F32), VMEM((2 * s.rep, s.cw), F32), VMEM((rows, width), F32), VMEM((rows, 128), F32),
            VMEM((3, width, 8 * s.hm), BF16), VMEM((rows // 8, 8 * s.hm, 8 * (FIN + 2)), BF16),
            VMEM((rows // 8, 24, 8 * s.hm), BF16), VMEM((4, 8, s.hid), F32),
            VMEM((rows, 8 * s.q), F32),
        ] + [VMEM(o.shape, o.dtype) for o in outs],
        compiler_params=pltpu.CompilerParams(collective_id=0, has_side_effects=True, vmem_limit_bytes=LIMIT),
        name="step",
    )(*args)
    update, row_new, col_new, hidden_new, cell_new = pl.pallas_call(
        put_out,
        out_shape=outs,
        in_specs=[ANY] * 5,
        out_specs=(ANY,) * 5,
        scratch_shapes=[VMEM(o.shape, o.dtype) for o in outs] + [sems(5)],
        compiler_params=pltpu.CompilerParams(vmem_limit_bytes=LIMIT),
        name="out",
    )(*made)
    return update, row_new.reshape(rows), col_new, hidden_new, cell_new


def solution(mesh):
    rowwise, owned, everywhere = P(("fsdp", "rep"), None), P("fsdp", None), P()

    def step(params, grads, moments, row_acc, lengths, tensor_order, col_acc, hidden_state, cell_state, *weights):
        s = Sizes(mesh, params, col_acc, hidden_state, weights[-1])
        return jax.shard_map(
            functools.partial(on_device, s),
            mesh=mesh,
            in_specs=(rowwise, rowwise, P(None, ("fsdp", "rep"), None), P(("fsdp", "rep")), everywhere, everywhere,
                      owned, owned, owned) + (everywhere,) * 5,
            out_specs=(rowwise, P(("fsdp", "rep")), owned, owned, owned),
            check_vma=False,
        )(params, grads, moments, row_acc, lengths, tensor_order, col_acc, hidden_state, cell_state, *weights)

    return step
```

```python
import functools
import math

import jax
import jax.numpy as jnp
from jax import lax
from jax.experimental import pallas as pl
from jax.experimental.pallas import tpu as pltpu
from jax.sharding import PartitionSpec as P

EPS = 1e-06
DECAY = 0.9
FIN = 8
F32 = jnp.float32
BF16 = jnp.bfloat16
MESH = pl.DeviceIdType.MESH
VMEM = pltpu.VMEM
LIMIT = 60 * 1024 * 1024
ANY = pl.BlockSpec(memory_space=pltpu.HBM)


class Sizes:
    def __init__(self, mesh, params, col_acc, hidden_state, rest):
        self.fsdp, self.rep = mesh.shape["fsdp"], mesh.shape["rep"]
        self.nz = self.ny = math.isqrt(self.fsdp)
        self.nt = col_acc.shape[0]
        self.own = self.nt // self.fsdp
        self.rows = params.shape[0] // (self.fsdp * self.rep)
        self.c = params.shape[1]
        self.hid = hidden_state.shape[1]
        self.hm = rest.shape[1] // 4
        self.sl = self.c // (self.rep - 1)
        self.cw = self.c + 128
        self.q = -(-(self.c + 3 * self.hid) // 1024) * 128
        self.all_rows = self.rows + 8
        assert self.own == 2 and self.sl % 128 == 0 and self.rows % 16 == 0


def iota(shape, dim):
    return lax.broadcasted_iota(jnp.int32, shape, dim)


def fiota(shape, dim):
    return iota(shape, dim).astype(F32)


def rem(a, b):
    return lax.rem(a, jnp.int32(b))


def div(a, b):
    return lax.div(a, jnp.int32(b))


def slot_bounds(s, lens, order):
    a, b = iota((s.nt, s.nt), 0), iota((s.nt, s.nt), 1)
    lens_col = jnp.sum(jnp.where(a == b, lens, 0.0), axis=1, keepdims=True)
    ids = a.astype(F32)
    end = jnp.sum(jnp.where(ids <= order, lens_col, 0.0), axis=0, keepdims=True)
    size = jnp.sum(jnp.where(ids == order, lens_col, 0.0), axis=0, keepdims=True)
    return end - size, end


def slot_hits(pos, start, end):
    return jnp.where((pos >= start) & (pos < end), 1.0, 0.0)


def ranges(pos, start, end):
    hits = slot_hits(pos, start, end)
    first = jnp.sum(hits * start, axis=1, keepdims=True)
    last = jnp.sum(hits * end, axis=1, keepdims=True)
    return first, last, hits


def split2(x):
    hi = x.astype(BF16)
    return hi, (x - hi.astype(F32)).astype(BF16)


def restack(t):
    lane = iota(t.shape, 1)
    both = t + pltpu.roll(t, 120, 1)
    hi = both.astype(BF16).astype(F32)
    low = pltpu.roll(both - hi, 8, 1)
    return jnp.where(lane < 8, hi, jnp.where(lane < 16, low, 0.0))


def remote(src, dst, send_sem, recv_sem, fsdp, rep):
    return pltpu.make_async_remote_copy(
        src_ref=src, dst_ref=dst, send_sem=send_sem, recv_sem=recv_sem,
        device_id={"fsdp": fsdp, "rep": rep}, device_id_type=MESH,
    )


def log_features(means, col_mean, col_square):
    feats = [jnp.log(means[k] + EPS) for k in range(5)]
    feats += [means[5] / jnp.sqrt(means[0] * means[1] + EPS), means[6] / jnp.sqrt(means[0] * means[3] + EPS),
              means[7] / jnp.sqrt(means[1] * means[3] + EPS), jnp.log(col_mean + EPS),
              jnp.log(col_square / (col_mean * col_mean))]
    return [v.astype(BF16).astype(F32) for v in feats]


def cell_step(s, feats, rec, w_in, bias, old):
    def gate(k):
        lo, hi = k * s.hid, (k + 1) * s.hid
        out = rec(k) + bias[:, lo:hi]
        w = w_in[:, lo:hi].astype(F32)
        for i, v in enumerate(feats):
            out = out + v * w[i : i + 1]
        return out

    now = jax.nn.sigmoid(gate(1)) * old + jax.nn.sigmoid(gate(0)) * jnp.tanh(gate(2))
    return jax.nn.sigmoid(gate(3)) * jnp.tanh(now), now


def kernel(s, params_h, grads_h, moments_h, row_acc_h, lens_h, order_h, col_acc_h, hidden_h, cell_h, w_in_h, w_rec_h,
           bias_h, w_first_h, w_rest_h,
           update_h, row_new_h, col_new_h, hidden_new_h, cell_new_h,
           params, grads, moments, row_acc, lens_i, order_i, col_acc, hidden, cell, w_in, w_rec, bias, w_first, w_rest,
           s_in, s_big, s_w, s_out,
           gs, ht, ag, htall, nb, table, nbsrc, gx, zsrc, zbuf, ysrc, ybuf,
           sent, one_come, p_come, t_come, y_come,
           cols, ht16, gen, scales, pick_w2, net1, net2, own_rec, held, update, row_new, col_new, hidden_new, cell_new):
    f, r = lax.axis_index("fsdp"), lax.axis_index("rep")
    z, y, core = div(f, s.ny), rem(f, s.ny), rem(r, 2)
    partner = r + 1 - 2 * core
    nxt, prv = rem(f + 1, s.fsdp), rem(f + s.fsdp - 1, s.fsdp)
    rows, nt, chunks, per = s.rows, s.nt, s.rep - 1, 2 * s.ny
    reps, ys, zs = range(1, s.rep), range(1, s.ny), range(1, s.nz)

    def at_rep(k):
        return rem(r + k, s.rep)

    def at_y(k):
        return z * s.ny + rem(y + k, s.ny)

    def at_z(k):
        return rem(z + k, s.nz) * s.ny + y

    ht_k, g_k, z_k, d_k, nb_k, p_k, t_k, y_k, y0_k = range(9)

    def all_come(ref, kind, fsdp, rep):
        remote(ref, ref, sent.at[kind], one_come.at[kind], fsdp, rep).wait_recv()

    def first_axis(k):
        return (1 - core) * at_y(k) + core * at_z(k)

    def second_axis(k):
        return (1 - core) * at_z(k) + core * at_y(k)

    with jax.named_scope("greet"):
        def fetch(pairs, sem):
            made = [pltpu.make_async_copy(a, b, sem.at[i]) for i, (a, b) in enumerate(pairs)]
            for c in made:
                c.start()
            return made

        small = fetch([(col_acc_h, col_acc), (hidden_h, hidden), (cell_h, cell), (lens_h, lens_i), (order_h, order_i),
                       (row_acc_h, row_acc)], s_in)
        big = fetch([(grads_h, grads)] + [(moments_h.at[k], moments.at[k]) for k in range(3)] + [(params_h, params)], s_big)
        barrier = pltpu.get_barrier_semaphore()
        peers = [(at_z(k), 2 * x) for k in zs for x in range(s.rep // 2)]
        peers += [(at_y(k), 2 * x + 1) for k in ys for x in range(s.rep // 2)]
        peers += [(f, at_rep(k)) for k in reps] + [(first_axis(k), r) for k in ys] + [(nxt, r), (prv, r)]
        for pf, pr in peers:
            pl.semaphore_signal(barrier, inc=1, device_id={"fsdp": pf, "rep": pr}, device_id_type=MESH)
    def fetch_weights():
        return fetch([(w_rec_h, w_rec), (w_in_h, w_in), (bias_h, bias), (w_first_h, w_first), (w_rest_h, w_rest)], s_w)

    with jax.named_scope("own"):
        for c in small[:3]:
            c.wait()
        own = jnp.concatenate([v.astype(BF16) for v in (col_acc[...], hidden[...])] + list(split2(cell[...])), axis=1)
        if s.c + 3 * s.hid < 8 * s.q:
            own = jnp.concatenate([own, jnp.zeros((2, 8 * s.q - s.c - 3 * s.hid), BF16)], axis=1)
        own = own.astype(F32)
        for half in range(2):
            parts = [own[:, (4 * half + q) * s.q : (4 * half + q + 1) * s.q] for q in range(4)]
            ag[half] = jnp.concatenate(parts, axis=0).astype(BF16)
    with jax.named_scope("meet"):
        pl.semaphore_wait(barrier, len(peers))
        c_p = {k: remote(ag.at[core], table.at[core, 0, k], sent.at[p_k], p_come.at[k], first_axis(k), r) for k in ys}
        near = sorted(zs, key=lambda k: min(k, s.nz - k))
        ring = s.nz == 8
        early = (0, 1, 7, 2, 6) if ring else ()
        t_two = {}

        def hop(src, slot, piece, to):
            sem = t_come.at[8 + 2 * piece + (slot == 6)] if slot in (2, 6) and piece in early else t_come.at[slot]
            c = remote(src, table.at[core, slot, piece], sent.at[t_k], sem, second_axis(to), r)
            c.start()
            return c

        def pass_on(piece, src):
            for k in (2, 6, 1, 7) if piece in early else near:
                t_two[k, piece] = hop(src, k, piece, k)

        def relay(piece):
            t_two[2, piece].wait_recv()
            if piece % 2 == 0:
                hop(table.at[core, 2, piece], 4, piece, 2)
            hop(table.at[core, 2, piece], 3, piece, 1)
            t_two[6, piece].wait_recv()
            if piece % 2 == 1:
                hop(table.at[core, 6, piece], 4, piece, 6)
            hop(table.at[core, 6, piece], 5, piece, 7)

        for k in near[::-1]:
            c_p[k].start()
        pass_on(0, ag.at[core])
        table[core, 0, 0] = ag[core]

    with jax.named_scope("stats"):
        for c in big:
            c.wait()
        sums = [jnp.zeros((rows, 1), F32) for _ in range(8)]
        for j in range(chunks):
            cs = pl.ds(j * s.sl, s.sl)
            g, p = grads[:, cs].astype(F32), params[:, cs]
            m = [moments[k, :, cs].astype(F32) for k in range(3)]
            sq = g * g
            gs[j] = sq.astype(BF16)
            for k, v in enumerate((sq, m[0] * m[0], m[1] * m[1], m[2] * m[2], p * p, g * m[0], g * m[2], m[0] * m[2])):
                sums[k] = sums[k] + jnp.sum(v, axis=1, keepdims=True)
        lane = iota((rows, 128), 1)
        stats = jnp.zeros((rows, 128), F32)
        for k in range(8):
            hi, low = split2(sums[k])
            stats = jnp.where(lane == k, hi.astype(F32), stats)
            stats = jnp.where(lane == k + 8, low.astype(F32), stats)
        gs[chunks] = jnp.zeros((rows, s.sl), BF16)
        gs[chunks, :, :128] = stats.astype(BF16)
    with jax.named_scope("send1"):
        c_g = [remote(gs.at[at_rep(k)], gx.at[k], sent.at[g_k], one_come.at[g_k], f, at_rep(k)) for k in reps]
        for c in c_g:
            c.start()
        weights = fetch_weights()
    with jax.named_scope("ends"):
        for c in small[3:]:
            c.wait()
        lens, order = lens_i[...].astype(F32), order_i[...].astype(F32)
        start, end = slot_bounds(s, lens, order)
        base = ((f * s.rep + r) * rows).astype(F32)
        which = fiota((16, 1), 0)
        pos = jnp.where(which == 0.0, base, jnp.where(which == 1.0, base + (rows - 1), -1.0))
        first, last, _ = ranges(pos, start, end)
        here = base + fiota((1, rows), 1)
        pick = slot_hits(here, first, last).astype(BF16)
        for j in range(chunks):
            part = jnp.dot(pick, gs[j], preferred_element_type=F32)
            ht[:, j * s.sl : (j + 1) * s.sl] = part[:2].astype(BF16)
        part = jnp.dot(pick, gs[chunks, :, :128], preferred_element_type=F32)
        ht[:, s.c :] = restack(part)[:2].astype(BF16)
        c_ht = [remote(ht, htall.at[k], sent.at[ht_k], one_come.at[ht_k], f, at_rep(k)) for k in reps]
        for c in c_ht:
            c.start()
        htall[0] = ht[...]
        gx[0] = gs[r]
        a, b = iota((rows, rows), 0), iota((rows, rows), 1)
        acc_col = jnp.sum(jnp.where(a == b, row_acc[...], 0.0), axis=1, keepdims=True)
        new_col = DECAY * acc_col + (1.0 - DECAY) * (sums[0] / s.c)
        row_new[...] = jnp.sum(jnp.where(a == b, new_col, 0.0), axis=0, keepdims=True)
        scales[:, 4:5] = new_col

    group = (f * (s.rep * rows)).astype(F32)
    which = fiota((8, 1), 0)
    first, last, _ = ranges(jnp.where(which == 0.0, group + (s.rep * rows - 1), group), start, end)
    coef = []
    for k in range(s.rep):
        at = group + (rem(r + s.rep - k, s.rep) * rows).astype(F32)
        head = jnp.where((at >= first) & (at < last), 1.0, 0.0)
        tail = jnp.where((at + (rows - 1) >= first) & (at + (rows - 1) < last), 1.0, 0.0)
        coef.append((head, tail * (1.0 - head)))

    width, m, taps = (FIN + 4) * s.hm, 8 * s.hm, 8 * (FIN + 2)
    lw = iota((m, width), 1)
    spread = jnp.where(rem(iota((m, 8), 0), 8) == iota((m, 8), 1), 1.0, 0.0).astype(BF16)
    keep = (rem(lw, s.hm) == div(iota((m, width), 0), 8)) & (lw < (FIN + 1) * s.hm)
    fold = jnp.where(div(iota((width, taps), 0), s.hm) == div(iota((width, taps), 1), 8), 1.0, 0.0).astype(BF16)
    diag1 = (rem(iota((m, taps), 0), 8) == rem(iota((m, taps), 1), 8)) & (iota((m, taps), 1) < 8 * (FIN + 1))
    diag2 = iota((8, m), 0) == rem(iota((8, m), 1), 8)
    for o in range(3):
        want = (FIN + 1) * s.hm + 3 * div(iota((width, m), 1), 8) + o
        pick_w2[o] = jnp.where(iota((width, m), 0) == want, 1.0, 0.0).astype(BF16)

    with jax.named_scope("wait_p"):
        then = {6: (0,)} if ring else {}
        for k in near:
            c_p[k].wait_recv()
            pass_on(k, table.at[core, 0, k])
            for piece in then.get(k, ()):
                relay(piece)
    with jax.named_scope("wait_g"):
        a, b = iota((nt, nt), 0), iota((nt, nt), 1)
        k1, p2, j2 = div(a, per), rem(div(a, 2), s.nz), rem(a, 2)
        slot = (1 - core) * (p2 * per + rem(y + k1, s.ny) * 2 + j2) + core * (rem(z + k1, s.nz) * per + p2 * 2 + j2)
        order_col = jnp.sum(jnp.where(b == slot, order, 0.0), axis=1, keepdims=True)
        ids = b.astype(F32)
        end_col = jnp.sum(jnp.where(ids <= order_col, lens, 0.0), axis=1, keepdims=True)
        start_col = end_col - jnp.sum(jnp.where(ids == order_col, lens, 0.0), axis=1, keepdims=True)
        all_come(gx.at[pl.ds(1, s.rep - 1)], g_k, f, r)
        part = jnp.zeros((nt, s.sl), F32)
        for k in range(s.rep):
            at = group + (rem(r + s.rep - k, s.rep) * rows).astype(F32) + fiota((1, rows), 1)
            part = part + jnp.dot(slot_hits(at, start_col, end_col).astype(BF16), gx[k], preferred_element_type=F32)
        for k in range(s.nz):
            zsrc[k] = part[k * per : (k + 1) * per].astype(BF16)
        c_z = [remote(zsrc.at[k], zbuf.at[k], sent.at[z_k], one_come.at[z_k], first_axis(k), r) for k in zs]
        for c in c_z:
            c.start()
        zbuf[0] = zsrc[0]
    with jax.named_scope("relay"):
        for piece in (1, 7, 2, 6) if ring else ():
            relay(piece)
        c_d = [remote(table.at[core, k], table.at[core, k], sent.at[d_k], one_come.at[d_k], f, partner) for k in range(s.nz)]
        c_d[0].start()
    with jax.named_scope("wait_ht"):
        all_come(htall.at[pl.ds(1, s.rep - 1)], ht_k, f, r)
        acc = jnp.zeros((2, s.cw), F32)
        for k in range(s.rep):
            both = htall[k].astype(F32)
            acc = acc + coef[k][0][:2] * both[0:1] + coef[k][1][:2] * both[1:2]
            ht16[2 * k : 2 * k + 2, :] = both
        acc = jnp.concatenate([acc[:, : s.c], restack(acc[:, s.c :])], axis=1)
        nbsrc[0] = jnp.broadcast_to(acc[0:1], (2, s.cw)).astype(BF16)
        nbsrc[1] = jnp.broadcast_to(acc[1:2], (2, s.cw)).astype(BF16)
        c_nb = [remote(nbsrc.at[i], nb.at[i], sent.at[nb_k], one_come.at[nb_k + 4 + i], to, r) for i, to in enumerate((nxt, prv))]
        for c in c_nb:
            c.start()

    n = s.all_rows
    row = iota((n, 1), 0)
    pos = jnp.where(row < rows, base + row.astype(F32), -1.0)
    lane = iota((n, nt), 1)
    hits = slot_hits(pos, start, end)
    hits = hits + jnp.where((row >= rows) & (row < rows + 2) & (lane == row - rows + 2 * f), 1.0, 0.0)
    first = jnp.sum(hits * start, axis=1, keepdims=True)
    last = jnp.sum(hits * end, axis=1, keepdims=True)
    length = jnp.maximum(last - first, 1.0)
    slot_of = jnp.sum(hits * lane.astype(F32), axis=1, keepdims=True)[:rows]
    first, last = first[:rows], last[:rows]
    same = slot_hits(base + fiota((1, rows), 1), first, last).astype(BF16)
    la = iota((1, 2 * s.rep), 1)
    head = group + (rem(r + s.rep - div(la, 2), s.rep) * rows).astype(F32)
    in_head = slot_hits(head, first, last)
    in_tail = slot_hits(head + (rows - 1), first, last) * (1.0 - in_head)
    shared = jnp.where(div(la, 2) == 0, 0.0, jnp.where(rem(la, 2) == 0, in_head, in_tail)).astype(BF16)
    before = slot_hits(group - 1.0, first, last)
    after = slot_hits(group + s.rep * rows, first, last)
    deep = s.nz * s.ny * 8
    lane = iota((rows, deep), 1)
    k2, k1, q4, j2 = div(lane, 8 * s.ny), rem(div(lane, 8), s.ny), rem(div(lane, 2), 4), rem(lane, 2)
    picks = []
    for half in range(2):
        kz, ky = (k2, k1) if half == 0 else (k1, k2)
        slot = rem(z + s.nz - kz, s.nz) * per + rem(y + s.ny - ky, s.ny) * 2 + j2
        hit = slot.astype(F32) == slot_of
        picks.append(jnp.concatenate([jnp.where(hit & (q4 == q), 1.0, 0.0) for q in range(4)], axis=0).astype(BF16))
    top = iota((8, 1), 0)

    def own_rows(v):
        return jnp.where(top == 0, v[0:1], jnp.where(top == 1, v[1:2], 0.0))

    def full_sums(g, lo, hi):
        out = jnp.dot(same, g, preferred_element_type=F32)
        out = out + jnp.dot(shared, ht16[:, lo:hi].astype(BF16), preferred_element_type=F32)
        return out + before * nb[0, :, lo:hi].astype(F32)[0:1] + after * nb[1, :, lo:hi].astype(F32)[0:1]

    def got_block(k):
        ref = table.at[core, k, pl.ds(3, 3)] if ring and k in (2, 6) else table.at[core, k]
        remote(ref, ref, sent.at[t_k], t_come.at[k], f, r).wait_recv()
        c_d[k].start()

    with jax.named_scope("wait_t"):
        for k in near:
            got_block(k)
    with jax.named_scope("wait_nb"):
        for c in c_nb:
            c.wait_recv()
        size = length[:rows]
        for j in range(chunks):
            lo, hi = j * s.sl, (j + 1) * s.sl
            cols[:, lo:hi] = full_sums(gs[j], lo, hi) * ((1.0 - DECAY) / size)
        stats = full_sums(gs[chunks, :, :128], s.c, s.cw)
        means = [(stats[:, k : k + 1] + stats[:, k + 8 : k + 9]) / (size * s.c) for k in range(8)]
    with jax.named_scope("wait_z"):
        all_come(zbuf.at[pl.ds(1, s.nz - 1)], z_k, f, r)
        total = zbuf[0].astype(F32)
        for k in zs:
            total = total + zbuf[k].astype(F32)
        total = total.astype(BF16)
        for k in range(s.ny):
            ysrc[k] = total[2 * k : 2 * k + 2]
        second = (1 - core) * z + core * y
        c_y = []
        for a in range(s.ny):
            for b in range(s.rep):
                if a or b:
                    c_y.append(remote(ysrc.at[rem(second + a, s.ny)], ybuf.at[a, r], sent.at[y_k if a else y0_k],
                                      y_come.at[a if a else s.ny + b], second_axis(a), at_rep(b)))
        for c in c_y:
            c.start()
        ybuf[0, r] = ysrc[second]

    with jax.named_scope("wait_d"):
        all_come(table.at[1 - core], d_k, f, partner)

    with jax.named_scope("rows"):
        for half in range(2):
            got = jnp.dot(picks[half], table[half].reshape(deep, s.q), preferred_element_type=F32)
            for q in range(4):
                held[:, (4 * half + q) * s.q : (4 * half + q + 1) * s.q] = got[q * rows : (q + 1) * rows]
        total_col = jnp.zeros((rows, 1), F32)
        total_sq = jnp.zeros((rows, 1), F32)
        for j in range(chunks):
            lo, hi = j * s.sl, (j + 1) * s.sl
            new = DECAY * held[:, lo:hi] + cols[:, lo:hi]
            cols[:, lo:hi] = new
            total_col = total_col + jnp.sum(new, axis=1, keepdims=True)
            total_sq = total_sq + jnp.sum(new * new, axis=1, keepdims=True)
        col_mean = total_col / s.c
        feats = log_features(means, col_mean, total_sq / s.c)
        for c in weights:
            c.wait()
        hid = jnp.concatenate([held[:, s.c : s.c + s.hid], own_rows(hidden[...])], axis=0).astype(BF16)
        old = held[:, s.c + s.hid : s.c + 2 * s.hid] + held[:, s.c + 2 * s.hid : s.c + 3 * s.hid]

        def rec(k):
            out = jnp.dot(hid, w_rec[:, k * s.hid : (k + 1) * s.hid], preferred_element_type=F32)
            own_rec[k] = out[rows:]
            return out[:rows]

        state, _ = cell_step(s, feats, rec, w_in, bias, old)
        bf = state.astype(BF16)
        gen[:, : FIN * s.hm] = jnp.dot(bf, w_first[...], preferred_element_type=F32)
        gen[:, FIN * s.hm :] = jnp.dot(bf, w_rest[...], preferred_element_type=F32)
        scales[:, 0:1] = scales[:, 4:5] / col_mean
        for i, k in enumerate((0, 1, 4)):
            scales[:, i + 1 : i + 2] = 1.0 / jnp.sqrt(means[k] + EPS)

    wide = s.c // 2 if s.c % 256 == 0 else s.c
    ones, zeros = jnp.ones((8, wide), F32), jnp.zeros((8, wide), F32)

    blocks = rows // 16
    outs = []

    with jax.named_scope("nets"):
        made = gen[...].astype(BF16).astype(F32)
        groups = [made[8 * i : 8 * i + 8].astype(BF16) for i in range(rows // 8)]
        wide1 = [jnp.where(keep, jnp.dot(spread, v, preferred_element_type=F32), 0.0).astype(BF16) for v in groups]
        for i, v in enumerate(wide1):
            net1[i] = jnp.where(diag1, jnp.dot(v, fold, preferred_element_type=F32), 0.0).astype(BF16)
        by_out = [jnp.dot(gen[...].astype(BF16), pick_w2[o], preferred_element_type=F32) for o in range(3)]
        for i in range(rows // 8):
            w2 = [jnp.where(diag2, v[8 * i : 8 * i + 8], 0.0) for v in by_out]
            net2[i] = jnp.concatenate(w2, axis=0).astype(BF16)

    def block(i):
        at = 16 * i
        sc = scales[at : at + 16, :]
        nets = [(net1[2 * i + half], net2[2 * i + half]) for half in range(2)]
        for j in range(s.c // wide):
            lo, hi = j * wide, (j + 1) * wide
            g16 = grads[at : at + 16, lo:hi].astype(F32)
            m16 = [moments[k, at : at + 16, lo:hi].astype(F32) for k in range(3)]
            p16 = params[at : at + 16, lo:hi]
            c16 = cols[at : at + 16, lo:hi]
            for half in range(2):
                q = slice(8 * half, 8 * half + 8)
                g, m0, m1, m2, p, cn = g16[q], m16[0][q], m16[1][q], m16[2][q], p16[q], c16[q]
                rms = lax.rsqrt(cn * sc[q, 0:1] + EPS)
                gn, mn = g * rms, m0 * rms
                x = jnp.concatenate(
                    [gn, mn, m1 * rms, m2 * rms, g * sc[q, 1:2], m0 * sc[q, 2:3], p * sc[q, 3:4], gn * mn, ones, zeros],
                    axis=0,
                ).astype(BF16)
                w1, w2 = nets[half]
                unit = jnp.maximum(jnp.dot(w1, x, preferred_element_type=F32), 0.0).astype(BF16)
                o = jnp.dot(w2, unit, preferred_element_type=F32)
                out = o[0:8] * jnp.exp(jnp.tanh(o[8:16])) * jax.nn.sigmoid(o[16:24])
                update[at + 8 * half : at + 8 * half + 8, lo:hi] = out

        c = pltpu.make_async_copy(update.at[pl.ds(at, 16)], update_h.at[pl.ds(at, 16)], s_out.at[i])
        c.start()
        outs.append(c)

    def owners():
        for a in ys:
            remote(ybuf.at[a], ybuf.at[a], sent.at[y_k], y_come.at[a], f, r).wait_recv()
        for c in c_y[: s.rep - 1]:
            c.wait_recv()
        size = length[rows:]

        def arrived(j):
            t = ybuf[0, j].astype(F32)
            for a in range(1, s.ny):
                t = t + ybuf[a, j].astype(F32)
            return own_rows(t)

        total_col = jnp.zeros((8, 1), F32)
        total_sq = jnp.zeros((8, 1), F32)
        for j in range(chunks):
            lo, hi = j * s.sl, (j + 1) * s.sl
            new = DECAY * own_rows(col_acc[:, lo:hi]) + (1.0 - DECAY) * arrived(j) / size
            col_new[:, lo:hi] = new[:2]
            total_col = total_col + jnp.sum(new, axis=1, keepdims=True)
            total_sq = total_sq + jnp.sum(new * new, axis=1, keepdims=True)
        stats = arrived(chunks)[:, :128]
        means = [(stats[:, k : k + 1] + stats[:, k + 8 : k + 9]) / (size * s.c) for k in range(8)]
        feats = log_features(means, total_col / s.c, total_sq / s.c)
        state, now = cell_step(s, feats, lambda k: own_rec[k], w_in, bias, own_rows(cell[...]))
        hidden_new[...] = state[:2]
        cell_new[...] = now[:2]
        for i, (a, b) in enumerate(((row_new, row_new_h), (col_new, col_new_h), (hidden_new, hidden_new_h), (cell_new, cell_new_h))):
            c = pltpu.make_async_copy(a, b, s_out.at[blocks + i])
            c.start()
            outs.append(c)

    for i in range(blocks):
        with jax.named_scope("block"):
            block(i)
    with jax.named_scope("owners"):
        owners()
    with jax.named_scope("drain"):
        def all_sent(ref, kind):
            remote(ref, ref, sent.at[kind], one_come.at[kind], f, r).wait_send()

        some, others = pl.ds(1, s.rep - 1), pl.ds(1, s.nz - 1)
        all_sent(htall.at[some], ht_k)
        all_sent(gx.at[some], g_k)
        all_sent(zbuf.at[others], z_k)
        all_sent(table.at[core], d_k)
        all_sent(nb, nb_k)
        all_sent(table.at[core, 0, others], p_k)
        all_sent(table.at[core, others], t_k)
        all_sent(ybuf.at[others], y_k)
        all_sent(ybuf.at[0, some], y0_k)
        for c in outs:
            c.wait()


def put_out(*refs):
    sems, rows = refs[15], refs[0].shape[0]
    here, there, held = ([v[0].at[pl.ds(i, 16)] for i in range(0, rows, 16)] + list(v[1:]) for v in (refs[:5], refs[5:10], refs[10:15]))
    come = [pltpu.make_async_copy(a, b, sems.at[0, i]) for i, (a, b) in enumerate(zip(here, held))]
    go = [pltpu.make_async_copy(a, b, sems.at[1, i]) for i, (a, b) in enumerate(zip(held, there))]
    for c in come:
        c.start()
    for a, b in zip(come, go):
        a.wait()
        b.start()
    for c in go:
        c.wait()


def on_device(s, params, grads, moments, row_acc, lengths, tensor_order, col_acc, hidden_state, cell_state,
              lstm_in, lstm_rec, lstm_bias, hyper_first, hyper_rest):
    shape = jax.ShapeDtypeStruct
    rows, per, width = s.rows, 2 * s.ny, (FIN + 4) * s.hm
    args = (params, grads, moments, row_acc.reshape(1, rows), lengths.reshape(1, s.nt), tensor_order.reshape(1, s.nt),
            col_acc, hidden_state, cell_state, lstm_in, lstm_rec, lstm_bias.reshape(1, -1), hyper_first, hyper_rest)

    def sems(k):
        return pltpu.SemaphoreType.DMA((2, k))

    def one(k):
        return pltpu.SemaphoreType.DMA((k,))

    outs = (
        shape(params.shape, F32), shape((1, rows), F32), shape(col_acc.shape, F32), shape(hidden_state.shape, F32),
        shape(cell_state.shape, F32),
    )
    made = pl.pallas_call(
        functools.partial(kernel, s),
        out_shape=outs,
        in_specs=[ANY] * len(args),
        out_specs=(ANY,) * 5,
        scratch_shapes=[VMEM(a.shape, a.dtype) for a in args] + [
            one(6), one(5), one(5), one(rows // 16 + 4),
            VMEM((s.rep, rows, s.sl), BF16), VMEM((2, s.cw), BF16), VMEM((2, 8, s.q), BF16),
            VMEM((s.rep, 2, s.cw), BF16), VMEM((2, 2, s.cw), BF16), VMEM((2, s.nz, s.ny, 8, s.q), BF16),
            VMEM((2, 2, s.cw), BF16), VMEM((s.rep, rows, s.sl), BF16),
            VMEM((s.nz, per, s.sl), BF16), VMEM((s.nz, per, s.sl), BF16), VMEM((s.ny, 2, s.sl), BF16),
            VMEM((s.ny, s.rep, 2, s.sl), BF16),
            one(9), one(10), one(s.ny), one(8 + 2 * s.ny), one(s.ny + s.rep),
            VMEM((rows, s.c), F32), VMEM((2 * s.rep, s.cw), F32), VMEM((rows, width), F32), VMEM((rows, 128), F32),
            VMEM((3, width, 8 * s.hm), BF16), VMEM((rows // 8, 8 * s.hm, 8 * (FIN + 2)), BF16),
            VMEM((rows // 8, 24, 8 * s.hm), BF16), VMEM((4, 8, s.hid), F32),
            VMEM((rows, 8 * s.q), F32),
        ] + [VMEM(o.shape, o.dtype) for o in outs],
        compiler_params=pltpu.CompilerParams(collective_id=0, has_side_effects=True, vmem_limit_bytes=LIMIT),
        name="step",
    )(*args)
    update, row_new, col_new, hidden_new, cell_new = pl.pallas_call(
        put_out,
        out_shape=outs,
        in_specs=[ANY] * 5,
        out_specs=(ANY,) * 5,
        scratch_shapes=[VMEM(o.shape, o.dtype) for o in outs] + [sems(rows // 16 + 4)],
        compiler_params=pltpu.CompilerParams(vmem_limit_bytes=LIMIT),
        name="out",
    )(*made)
    return update, row_new.reshape(rows), col_new, hidden_new, cell_new


def solution(mesh):
    rowwise, owned, everywhere = P(("fsdp", "rep"), None), P("fsdp", None), P()

    def step(params, grads, moments, row_acc, lengths, tensor_order, col_acc, hidden_state, cell_state, *weights):
        s = Sizes(mesh, params, col_acc, hidden_state, weights[-1])
        return jax.shard_map(
            functools.partial(on_device, s),
            mesh=mesh,
            in_specs=(rowwise, rowwise, P(None, ("fsdp", "rep"), None), P(("fsdp", "rep")), everywhere, everywhere,
                      owned, owned, owned) + (everywhere,) * 5,
            out_specs=(rowwise, P(("fsdp", "rep")), owned, owned, owned),
            check_vma=False,
        )(params, grads, moments, row_acc, lengths, tensor_order, col_acc, hidden_state, cell_state, *weights)

    return step
```
